32 devices in a mesh: blk: 4 (over y, x), grp: 8 (over z, core).
Axes of the slice: x: 2, y: 2, z: 4, core: 2. Of those that a mesh axis runs over, the one named last changes fastest.
Arguments:
- b3c: bfloat16 [384, 3, 32, 4096], P('blk', None, None, 'grp'), may hold values from -6 to 6
- green_occ: bfloat16 [384, 384], P('blk', 'grp'), may hold values from -0.3125 to 0.3125
- green_virt: bfloat16 [384, 384], P(None, 'grp'), may hold values from -0.625 to 0.625
- occ_mask: int32 [12, 12], replicated, may hold values from 0 to 1, as said below
- a_tiles: bfloat16 [128, 32, 1024], P(('blk', 'grp')), may hold values from -0.046875 to 0.046875
- tile_codes: int32 [128], P(('blk', 'grp')), may hold values from -1 to 143, as said below
Outputs:
- chi: float32 [512, 4096], P('blk', 'grp')
The draws below stay inside these ranges and needn't reach their ends.
Inputs may be any that keep to these rules, and one draw needn't show every extreme that they name: `occ_mask`: the diagonal is 1. `tile_codes`: each device's 4 slots hold its live tiles first and -1 after them; some device has all 4 slots live; codes may repeat, and repeated tiles add.
All inputs are finite; a program needn't handle non-finite values.
Results may differ from the reference program's by a relative error of at most 0.0041.
Values may be sent and summed in bfloat16 or wider, within the bound.
No kernel may reach another device: no remote copies, remote signals or barrier semaphores. Data moves between devices by JAX's collectives and lax.ppermute only.
A program may use at most 192 MiB of HBM per device.

```python
import jax
import jax.numpy as jnp
from jax import lax

BS = 32
PB = 32
QBATCH = 4096
KB = 3
BAND = 3
TSLOT = 4
NB = 384
NPB = 16
NAUX = 512
OWNERS = 32
N_BLK = 4
N_GRP = 8


def draw_occ_mask(key, part):
    block_total = KB * N_BLK
    first = jnp.arange(block_total, dtype=jnp.int32)[:, None]
    second = jnp.arange(block_total, dtype=jnp.int32)[None, :]
    coins = jax.random.randint(jax.random.fold_in(key, 11), (block_total, block_total), 0, 4)
    keep = (coins > 0) | (first == second)
    return keep.astype(jnp.int32)


def draw_tile_codes(key, part):
    owners = N_BLK * N_GRP
    heavy = jax.random.randint(jax.random.fold_in(key, 21), (owners,), 0, 4)
    light = jax.random.randint(jax.random.fold_in(key, 22), (owners,), 1, TSLOT // 2 + 1)
    counts = jnp.where(heavy == 0, TSLOT, light)
    forced = jax.random.randint(jax.random.fold_in(key, 23), (), 0, owners)
    counts = jnp.where(jnp.arange(owners, dtype=jnp.int32) == forced, TSLOT, counts)
    codes = jax.random.randint(jax.random.fold_in(key, 24), (owners, TSLOT), 0, NPB * KB * BAND)
    slots = jnp.arange(TSLOT, dtype=jnp.int32)[None, :]
    codes = jnp.where(slots < counts[:, None], codes, -1)
    return codes.reshape(owners * TSLOT).astype(jnp.int32)


def block_scale(own_key, extent, split, smallest, largest):
    gain, own = 1.0, jax.random.fold_in(own_key, 6)
    for axis_at, parts in split:
        heights = jnp.exp(jax.random.uniform(jax.random.fold_in(own, axis_at), (parts,), jnp.float32, smallest / len(split), largest / len(split)))
        gain = gain * jnp.repeat(heights, extent[axis_at] // parts).reshape([-1 if axis == axis_at else 1 for axis in range(len(extent))])
    return gain


def bell_draw(own_key, dims, width, limit, split=(), kind=jnp.bfloat16):
    result = jax.random.normal(own_key, dims, jnp.float32) * width
    if len(split) > 0:
        result = block_scale(own_key, dims, split, -0.22, 0.18) * result
    return jnp.clip(result, min=-limit, max=limit).astype(kind)


def setup_inputs(seed: int = 0) -> dict:
    splits = jax.random.split(jax.random.key(seed), 7)
    b3c = bell_draw(splits[0], (NB, BAND, BS, QBATCH), 1.0, 6.0, ((0, 4), (3, 8)))
    green_occ = bell_draw(splits[1], (NB, NB), NB ** -0.5, 0.3125, ((0, 4), (1, 8)))
    green_virt = bell_draw(splits[2], (NB, NB), (BAND * BS) ** -0.5, 0.625, ((1, 8),))
    occ_mask = draw_occ_mask(jax.random.fold_in(splits[6], 71), 0)
    a_tiles = bell_draw(splits[4], (OWNERS * TSLOT, PB, BS * BS), (BS * BS * 16) ** -0.5, 0.046875, ((0, 32),))
    tile_codes = draw_tile_codes(jax.random.fold_in(splits[6], 71), 0)
    return dict(b3c=b3c, green_occ=green_occ, green_virt=green_virt, occ_mask=occ_mask, a_tiles=a_tiles, tile_codes=tile_codes)


def reference(b3c, green_occ, green_virt, occ_mask, a_tiles, tile_codes):
    block_total = KB * N_BLK
    basis_total = block_total * BS
    window = (KB + BAND - 1) * BS
    pair_count = KB * BAND
    mask_full = jnp.repeat(jnp.repeat(occ_mask, BS, axis=0), BS, axis=1).astype(jnp.bfloat16)
    masked_occ = green_occ * mask_full
    partner_blocks = (jnp.arange(block_total, dtype=jnp.int32)[:, None] + jnp.arange(BAND, dtype=jnp.int32)[None, :]) % block_total
    span = min(512, QBATCH)
    span_count = QBATCH // span
    group_pairs = []
    for group in range(N_BLK):
        rows = (group * KB * BS + jnp.arange(window, dtype=jnp.int32)) % basis_total
        virt_rows = jnp.take(green_virt, rows, axis=0).reshape(window, block_total, BS)
        virt_sel = jnp.take(virt_rows, partner_blocks, axis=1).astype(jnp.float32)
        occ_rows = masked_occ[group * KB * BS:(group + 1) * KB * BS]

        def one_span(index):
            tensor = lax.dynamic_slice_in_dim(b3c, index * span, span, 3)
            tensor = tensor.reshape(block_total, BS, BAND, BS, span).astype(jnp.float32)
            inner = jnp.einsum('wlds,ladsq->lawq', virt_sel, tensor, precision=lax.Precision.HIGHEST).astype(jnp.bfloat16)
            product = jnp.dot(occ_rows, inner.reshape(basis_total, window * span), preferred_element_type=jnp.float32)
            return product.reshape(KB * BS, window, span)

        spans = lax.map(one_span, jnp.arange(span_count, dtype=jnp.int32))
        paired = jnp.moveaxis(spans, 0, 2).reshape(KB * BS, window, QBATCH).astype(jnp.bfloat16)
        pieces = []
        for block in range(KB):
            for offset in range(BAND):
                piece = paired[block * BS:(block + 1) * BS, (block + offset) * BS:(block + offset + 1) * BS]
                pieces.append(piece.reshape(BS * BS, QBATCH))
        group_pairs.append(jnp.stack(pieces))
    pairs_all = jnp.stack(group_pairs)
    slot_groups = (jnp.arange(OWNERS * TSLOT, dtype=jnp.int32) // (N_GRP * TSLOT)).astype(jnp.int32)

    def add_tile(total, items):
        tile, code, group = items
        valid = code >= 0
        pair = jnp.where(valid, code % pair_count, 0).astype(jnp.int32)
        pblock = jnp.where(valid, code // pair_count, 0).astype(jnp.int32)
        values = pairs_all[group, pair]
        contrib = jnp.dot(tile, values, preferred_element_type=jnp.float32) * valid.astype(jnp.float32)
        start = (pblock * PB).astype(jnp.int32)
        current = lax.dynamic_slice_in_dim(total, start, PB, 0)
        return lax.dynamic_update_slice_in_dim(total, current + contrib, start, 0), None

    initial = jnp.zeros((NAUX, QBATCH), jnp.float32)
    chi, _ = lax.scan(add_tile, initial, (a_tiles, tile_codes, slot_groups))
    return chi
```

```python
import functools

import jax
import jax.numpy as jnp
from jax import lax
from jax.experimental import pallas as pl
from jax.experimental.pallas import tpu as pltpu
from jax.sharding import PartitionSpec as P

BS = 32
PB = 32
KB = 3
BAND = 3
PBD = 4
LANES = 128
PACK = 4


def transform_kernel(nu_blocks, gv_ref, go_ref, b_ref, out_ref, *scratch):
    part = pl.program_id(1)
    rows, cols = gv_ref.shape[1], b_ref.shape[2]
    lam = b_ref.shape[0]
    for block in range(lam // BS):

        def first(i, carry):
            at = block * BS + i
            r = jnp.dot(gv_ref[block], b_ref[at], preferred_element_type=jnp.float32)
            for c, s in enumerate(scratch):
                s[pl.ds(at, rows, stride=lam), :] = r[:, c * LANES : (c + 1) * LANES]
            return carry

        lax.fori_loop(0, BS, first, 0)
    for nb in range(nu_blocks):
        start = pl.multiple_of((part * nu_blocks + nb) * BS, BS)
        occ = go_ref[pl.ds(start, BAND * BS), :]

        def second(i, carry):
            at = pl.multiple_of((nb * BS + i) * lam, lam)
            w = jnp.concatenate([s[pl.ds(at, lam), :] for s in scratch], axis=1)
            r = jnp.dot(occ, w.astype(jnp.bfloat16), preferred_element_type=jnp.float32)
            r = r.astype(jnp.bfloat16)
            to = pl.multiple_of(i * BS, BS)
            for j in range(BAND):
                out_ref[nb, BAND - 1 - j, pl.ds(to, BS), :] = r[j * BS : (j + 1) * BS]
            return carry

        lax.fori_loop(0, BS, second, 0)


def transform(b, gv, go):
    lam, band, q = b.shape
    nb_total = gv.shape[1] // BS
    cols = min(2 * LANES, q)
    nu_blocks = 6
    parts = nb_total // nu_blocks
    rows = nu_blocks * BS
    return pl.pallas_call(
        functools.partial(transform_kernel, nu_blocks),
        grid=(q // cols, parts),
        in_specs=[
            pl.BlockSpec((lam // BS, rows, band), lambda i, j: (0, j, 0)),
            pl.BlockSpec(go.shape, lambda i, j: (0, 0)),
            pl.BlockSpec((lam, band, cols), lambda i, j: (0, 0, i)),
        ],
        out_specs=pl.BlockSpec((nu_blocks, BAND, BS * BS, cols), lambda i, j: (j, 0, 0, i)),
        out_shape=jax.ShapeDtypeStruct((nb_total, BAND, BS * BS, q), jnp.bfloat16),
        scratch_shapes=[pltpu.VMEM((rows * lam, LANES), jnp.float32)] * (cols // LANES),
        compiler_params=pltpu.CompilerParams(vmem_limit_bytes=60 * 2**20),
        cost_estimate=pl.CostEstimate(
            flops=4 * lam * band * nb_total * BS * q, bytes_accessed=100 * 2**20, transcendentals=0
        ),
        name="transform",
    )(gv, go, b)


def tiles_kernel(pair_ref, slot_ref, row_ref, count_ref, *refs):
    tiles, (paired_ref, out_ref, acc) = refs[:PACK], refs[PACK:]
    step = pl.program_id(0)

    @pl.when(step == 0)
    def _():
        acc[...] = jnp.zeros_like(acc)

    @pl.when(step < count_ref[0])
    def _():
        lhs = jnp.concatenate([t[0] for t in tiles], axis=0)
        r = jnp.dot(lhs, paired_ref[0], preferred_element_type=jnp.float32)
        for t in range(PACK):
            at = row_ref[step * PACK + t]
            acc[at] += r[t * PB : (t + 1) * PB]

    @pl.when(step == pl.num_programs(0) - 1)
    def _():
        out_ref[...] = acc[: out_ref.shape[0]]


def contract(tiles, paired, pairs, slots, rows, count, aux):
    q = paired.shape[2]
    items = pairs.shape[0]

    def tile_spec(t):
        return pl.BlockSpec(
            (1, PB, BS * BS), lambda s, pair, slot, row, n: (slot[s * PACK + t], 0, 0)
        )

    return pl.pallas_call(
        tiles_kernel,
        grid_spec=pltpu.PrefetchScalarGridSpec(
            num_scalar_prefetch=4,
            grid=(items,),
            in_specs=[tile_spec(t) for t in range(PACK)]
            + [pl.BlockSpec((1, BS * BS, q), lambda s, pair, slot, row, n: (pair[s], 0, 0))],
            out_specs=pl.BlockSpec((aux, PB, q), lambda s, pair, slot, row, n: (0, 0, 0)),
            scratch_shapes=[pltpu.VMEM((aux + 1, PB, q), jnp.float32)],
        ),
        out_shape=jax.ShapeDtypeStruct((aux, PB, q), jnp.float32),
        compiler_params=pltpu.CompilerParams(vmem_limit_bytes=60 * 2**20),
        name="contract",
    )(pairs, slots, rows, count, *([tiles] * PACK), paired)


def schedule(pblock, pair, live, pair_total, aux):
    total = pair.shape[0]
    items = pair_total + total // PACK
    key = jnp.where(live, pair, pair_total)
    at = jnp.arange(total, dtype=jnp.int32)
    same = (key[:, None] == key[None, :]) & (at[None, :] < at[:, None])
    rank = jnp.sum(same, axis=1, dtype=jnp.int32)
    names = jnp.arange(pair_total, dtype=jnp.int32)
    number = jnp.sum(key[None, :] == names[:, None], axis=1, dtype=jnp.int32)
    groups = (number + PACK - 1) // PACK
    base = jnp.sum(jnp.where(names[None, :] < key[:, None], groups[None, :], 0), axis=1)
    place = jnp.where(live, (base + rank // PACK) * PACK + rank % PACK, -1)
    count = jnp.sum(groups, dtype=jnp.int32)
    hit = place[None, :] == jnp.arange(items * PACK, dtype=jnp.int32)[:, None]
    slots = jnp.sum(jnp.where(hit, at[None, :], 0), axis=1)
    rows = jnp.sum(jnp.where(hit, pblock[None, :] - aux, 0), axis=1) + aux
    start = jnp.cumsum(groups) - groups
    step = jnp.minimum(jnp.arange(items, dtype=jnp.int32), count - 1)
    pairs = jnp.max(
        jnp.where((start[None, :] <= step[:, None]) & (groups[None, :] > 0), names[None, :], 0),
        axis=1,
    )
    return pairs.astype(jnp.int32), slots.astype(jnp.int32), rows.astype(jnp.int32), count[None]


def local(b3c, green_occ, green_virt, occ_mask, a_tiles, tile_codes):
    n_blk, n_grp = lax.axis_size("blk"), lax.axis_size("grp")
    group = lax.axis_index("blk")
    lam, _, _, q = b3c.shape
    basis = green_virt.shape[0]
    blocks = basis // BS
    aux = n_blk * PBD
    slots_here = a_tiles.shape[0]

    turned = a_tiles.reshape(slots_here, PB, BS, BS).swapaxes(2, 3).reshape(a_tiles.shape)
    tiles = lax.all_gather(turned, ("blk", "grp"), axis=0, tiled=True)

    wide = green_occ.shape[1]
    quarter = lax.dynamic_slice_in_dim(green_virt, group * lam, lam, 0)
    pblock = jnp.where(tile_codes >= 0, tile_codes // (KB * BAND), -1)
    within = jnp.where(tile_codes >= 0, tile_codes % (KB * BAND), 0)
    coded = jnp.stack([pblock, within]).astype(jnp.bfloat16)
    coded = jnp.pad(coded, ((0, 14), (0, wide - slots_here)))
    sent = jnp.concatenate([green_occ, quarter, coded], axis=0)
    got = lax.all_gather(sent, ("blk", "grp"), axis=0, tiled=False)
    got = got.reshape(n_blk, n_grp, 2 * lam + 16, wide)
    whole = got[:, :, : 2 * lam].transpose(0, 2, 1, 3).reshape(n_blk, 2, lam, basis)
    occ_all = whole[:, 0].reshape(basis, basis)
    virt_all = whole[:, 1].reshape(basis, basis)
    codes = got[:, :, 2 * lam : 2 * lam + 2, :slots_here].astype(jnp.int32)
    pblock = codes[:, :, 0].reshape(-1)
    within = codes[:, :, 1].reshape(-1)

    mask = lax.dynamic_slice_in_dim(occ_mask, group * KB, KB, 1)
    mask = jnp.repeat(jnp.repeat(mask, BS, axis=0), BS, axis=1).astype(jnp.bfloat16)
    occ = lax.dynamic_slice_in_dim(occ_all, group * lam, lam, 1) * mask
    occ = jnp.concatenate([occ[-(BAND - 1) * BS :], occ], axis=0)
    virt = jnp.concatenate([virt_all, virt_all[:, : (BAND - 1) * BS]], axis=1)
    virt = lax.dynamic_slice_in_dim(virt, group * lam, lam + (BAND - 1) * BS, 1)
    virt = jnp.stack([virt[:, l * BS : (l + BAND) * BS] for l in range(KB)])

    paired = transform(b3c.reshape(lam, BAND * BS, q), virt, occ)
    paired = paired.reshape(blocks * BAND, BS * BS, q)

    owner = jnp.arange(pblock.shape[0], dtype=jnp.int32) // (n_grp * slots_here)
    offset = within % BAND
    nu = (owner * KB + within // BAND + offset) % blocks
    pairs, slots, rows, count = schedule(
        pblock, nu * BAND + offset, pblock >= 0, blocks * BAND, aux
    )
    chi = contract(tiles, paired, pairs, slots, rows, count, aux)
    chi = chi.reshape(n_blk, PBD * PB, q)

    total = lax.dynamic_index_in_dim(chi, group, 0, False)
    for d in range(1, n_blk):
        piece = lax.dynamic_index_in_dim(chi, (group + d) % n_blk, 0, False)
        moved = lax.ppermute(
            piece.astype(jnp.bfloat16), "blk", [(i, (i + d) % n_blk) for i in range(n_blk)]
        )
        total = total + moved.astype(jnp.float32)
    return total


def solution(mesh):
    in_specs = (
        P("blk", None, None, "grp"),
        P("blk", "grp"),
        P(None, "grp"),
        P(),
        P(("blk", "grp"), None, None),
        P(("blk", "grp")),
    )
    out_specs = P("blk", "grp")
    return jax.shard_map(local, mesh=mesh, in_specs=in_specs, out_specs=out_specs, check_vma=False)
```

```python
import functools

import jax
import jax.numpy as jnp
from jax import lax
from jax.experimental import pallas as pl
from jax.experimental.pallas import tpu as pltpu
from jax.sharding import PartitionSpec as P

BS = 32
PB = 32
KB = 3
BAND = 3
PBD = 4
LANES = 128
NU_PART = 6
UNROLL = 16


def transform_kernel(pitch, gv_ref, go_ref, b_ref, out_ref, *scratch):
    part = pl.program_id(0)
    rows = gv_ref.shape[1]
    lam = b_ref.shape[0]
    for block in range(lam // BS):

        def first(i, carry):
            at = block * BS + i
            r = jnp.dot(gv_ref[block], b_ref[at], preferred_element_type=jnp.float32)
            for c, s in enumerate(scratch):
                s[pl.ds(at, rows, stride=pitch), :] = r[:, c * LANES : (c + 1) * LANES]
            return carry

        lax.fori_loop(0, BS, first, 0, unroll=UNROLL)
    for nb in range(rows // BS):
        start = pl.multiple_of((part * (rows // BS) + nb) * BS, BS)
        occ = go_ref[pl.ds(start, BAND * BS), :]
        zero = jnp.zeros_like(occ)
        occ = jnp.concatenate(
            [jnp.concatenate([occ, zero], axis=1), jnp.concatenate([zero, occ], axis=1)], axis=0
        )

        def second(i, carry):
            at = (nb * BS + 2 * i) * pitch
            w = jnp.concatenate(
                [
                    jnp.concatenate([s[pl.ds(at, lam), :], s[pl.ds(at + pitch, lam), :]], axis=0)
                    for s in scratch
                ],
                axis=1,
            )
            r = jnp.dot(occ, w.astype(jnp.bfloat16), preferred_element_type=jnp.float32)
            r = r.astype(jnp.bfloat16)
            for h in range(2):
                to = pl.multiple_of((2 * i + h) * BS, BS)
                for j in range(BAND):
                    row = (h * BAND + j) * BS
                    out_ref[nb, BAND - 1 - j, pl.ds(to, BS), :] = r[row : row + BS]
            return carry

        lax.fori_loop(0, BS // 2, second, 0, unroll=UNROLL)


def transform(b, gv, go, cols, which):
    lam, band, q = b.shape
    nb_total = gv.shape[1] // BS
    parts = nb_total // NU_PART
    rows = NU_PART * BS
    pitch = lam + 2
    return pl.pallas_call(
        functools.partial(transform_kernel, pitch),
        grid=(parts,),
        in_specs=[
            pl.BlockSpec((lam // BS, rows, band), lambda j: (0, j, 0)),
            pl.BlockSpec(go.shape, lambda j: (0, 0)),
            pl.BlockSpec((lam, band, cols), lambda j: (0, 0, which)),
        ],
        out_specs=pl.BlockSpec((NU_PART, BAND, BS * BS, cols), lambda j: (j, 0, 0, 0)),
        out_shape=jax.ShapeDtypeStruct((nb_total, BAND, BS * BS, cols), jnp.bfloat16),
        scratch_shapes=[pltpu.VMEM((rows * pitch, LANES), jnp.float32)] * (cols // LANES),
        compiler_params=pltpu.CompilerParams(vmem_limit_bytes=60 * 2**20),
        cost_estimate=pl.CostEstimate(
            flops=150 * 10**8, bytes_accessed=24 * 2**20, transcendentals=0
        ),
        name="transform",
    )(gv, go, b)


def tiles_kernel(items, halves, first, nu_ref, slot_ref, row_ref, count_ref, *refs):
    near, far = refs[0], refs[1]
    paired = refs[2 : 2 + BAND * halves]
    out_ref = refs[-1]
    m = pl.program_id(0)

    @pl.when(m == 0)
    def _():
        if first:
            out_ref[...] = jnp.zeros_like(out_ref)
        else:
            out_ref[...] = refs[-2][...]

    for d in range(BAND):
        pair = m * BAND + d

        def item(i, carry):
            at = (pair * items + i) * 4
            lhs = jnp.concatenate(
                [near[slot_ref[at]], near[slot_ref[at + 1]], far[slot_ref[at + 2]], far[slot_ref[at + 3]]],
                axis=0,
            )
            for h in range(halves):
                rhs = paired[d * halves + h]
                r = jnp.dot(lhs, rhs[0, 0], preferred_element_type=jnp.float32)
                cols = rhs.shape[3]
                for t in range(4):
                    out_ref[row_ref[at + t], :, h * cols : (h + 1) * cols] += r[t * PB : (t + 1) * PB]
            return carry

        item(0, 0)
        lax.fori_loop(1, count_ref[pair], item, 0)


def contract(near, far, paired, nu, slots, rows, count, aux, total):
    halves = len(paired)
    cols = paired[0].shape[3]
    q = halves * cols
    items = slots.shape[0] // (KB * BAND * 4)
    first = total is None
    acc = pl.BlockSpec((aux + 1, PB, q), lambda m, *_: (0, 0, 0))
    whole = pl.BlockSpec(near.shape, lambda m, *_: (0, 0, 0))

    def paired_spec(d):
        return pl.BlockSpec(
            (1, 1, BS * BS, cols), lambda m, nu, *_: (nu[m * BAND + d], d, 0, 0)
        )

    return pl.pallas_call(
        functools.partial(tiles_kernel, items, halves, first),
        grid_spec=pltpu.PrefetchScalarGridSpec(
            num_scalar_prefetch=4,
            grid=(KB,),
            in_specs=[whole, whole]
            + [paired_spec(d) for d in range(BAND) for _ in range(halves)]
            + ([] if first else [acc]),
            out_specs=acc,
        ),
        out_shape=jax.ShapeDtypeStruct((aux + 1, PB, q), jnp.float32),
        compiler_params=pltpu.CompilerParams(vmem_limit_bytes=60 * 2**20),
        cost_estimate=pl.CostEstimate(
            flops=40 * 10**8, bytes_accessed=12 * 2**20, transcendentals=0
        ),
        name="contract",
    )(nu, slots, rows, count, near, far, *(list(paired) * BAND), *([] if first else [total]))


def schedule(codes, aux):
    groups, sides, total = codes.shape
    pairs = KB * BAND
    items = total // 2
    live = codes >= 0
    key = jnp.where(live, codes % pairs, pairs)
    at = jnp.arange(total, dtype=jnp.int32)
    same = (key[..., :, None] == key[..., None, :]) & (at[None, :] < at[:, None])
    rank = jnp.sum(same, axis=-1, dtype=jnp.int32)
    place = jnp.where(live, key * total + rank, -1)
    hit = place[..., None, :] == jnp.arange(pairs * total, dtype=jnp.int32)[:, None]
    slots = jnp.sum(jnp.where(hit, at, 0), axis=-1, dtype=jnp.int32)
    rows = aux + jnp.sum(jnp.where(hit, codes[..., None, :] // pairs - aux, 0), axis=-1, dtype=jnp.int32)

    def table(a):
        return a.reshape(groups, sides, pairs * items, 2).swapaxes(1, 2).reshape(groups, -1)

    number = jnp.sum(
        key[..., None, :] == jnp.arange(pairs, dtype=jnp.int32)[:, None], axis=-1, dtype=jnp.int32
    )
    count = (jnp.max(number, axis=1) + 1) // 2
    return table(slots), table(rows), count


def local(b3c, green_occ, green_virt, occ_mask, a_tiles, tile_codes):
    n_blk, n_grp = lax.axis_size("blk"), lax.axis_size("grp")
    group, member = lax.axis_index("blk"), lax.axis_index("grp")
    lam, _, _, q = b3c.shape
    basis, wide = green_virt.shape
    blocks = basis // BS
    aux = n_blk * PBD
    slots_here = a_tiles.shape[0]
    spread = n_grp // 2

    def grp_swap(a, bits):
        return lax.ppermute(a, "grp", [(i, i ^ bits) for i in range(n_grp)])

    def blk_swap(a, bits):
        return lax.ppermute(a, "blk", [(i, i ^ bits) for i in range(n_blk)])

    coded = jnp.stack([tile_codes // (KB * BAND), tile_codes % (KB * BAND)])
    coded = jnp.where(tile_codes >= 0, coded, -1).astype(jnp.bfloat16)
    coded = jnp.pad(coded, ((0, 14), (0, wide - slots_here)))
    small = jnp.concatenate([green_virt, green_occ, coded], axis=0)[None]
    bit = 2
    while bit < n_grp:
        small = jnp.concatenate([small, grp_swap(small, bit)], axis=0)
        bit *= 2
    small = jnp.concatenate([small, grp_swap(small, 1)], axis=0)
    relative = jnp.arange(n_grp, dtype=jnp.int32) ^ member
    order = (relative % 2) * spread + relative // 2
    ordered = jnp.take(small[:, : basis + lam], order, axis=0)
    virt_all = ordered[:, :basis].swapaxes(0, 1).reshape(basis, basis)
    occ_rows = ordered[:, basis:].swapaxes(0, 1).reshape(lam, basis)
    code = small[:, basis + lam : basis + lam + 2, :slots_here]
    code = jnp.where(code[:, 0] >= 0, code[:, 0] * (KB * BAND) + code[:, 1], -1)
    code = code.reshape(-1)
    code_rows = -(-code.shape[0] // lam)
    code_rows = -(-code_rows // 16) * 16
    part = jnp.stack([small[:, basis + lam, :slots_here], small[:, basis + lam + 1, :slots_here]])
    part = part.reshape(2, -1)
    part = jnp.pad(part, ((0, 0), (0, code_rows // 2 * lam - part.shape[1])))
    part = part.reshape(code_rows, lam)
    received = []
    for mask in range(n_blk):
        mine = lax.dynamic_slice_in_dim(occ_rows, (group ^ mask) * lam, lam, 1)
        packet = jnp.concatenate([mine, part], axis=0)
        received.append(blk_swap(packet, mask) if mask else packet)
    received = jnp.stack(received)
    occ = jnp.take(received[:, :lam], jnp.arange(n_blk, dtype=jnp.int32) ^ group, axis=0)
    occ = occ.reshape(basis, lam)
    part = received[:, lam:].reshape(n_blk, 2, -1)[:, :, : n_grp * slots_here]
    part = part.astype(jnp.int32)
    codes = jnp.where(part[:, 0] >= 0, part[:, 0] * (KB * BAND) + part[:, 1], -1)
    codes = codes.reshape(n_blk, 2, spread * slots_here)

    mask = lax.dynamic_slice_in_dim(occ_mask, group * KB, KB, 1)
    mask = jnp.repeat(jnp.repeat(mask, BS, axis=0), BS, axis=1).astype(jnp.bfloat16)
    occ = occ * mask
    occ = jnp.concatenate([occ[-(BAND - 1) * BS :], occ], axis=0)
    virt = jnp.concatenate([virt_all, virt_all[:, : (BAND - 1) * BS]], axis=1)
    virt = lax.dynamic_slice_in_dim(virt, group * lam, lam + (BAND - 1) * BS, 1)
    virt = jnp.stack([virt[:, l * BS : (l + BAND) * BS] for l in range(KB)])

    turned = a_tiles.reshape(slots_here, PB, BS, BS).swapaxes(2, 3).reshape(a_tiles.shape)
    near = {0: jnp.concatenate([turned] + [grp_swap(turned, 2 * d) for d in range(1, spread)])}
    for to in range(1, n_blk):
        low = to & -to
        if low == to:
            near[to] = blk_swap(near[0], to)
        else:
            high = 1 << (to.bit_length() - 1)
            half = near[0].shape[0] // 2
            near[to] = jnp.concatenate(
                [blk_swap(near[to ^ low][:half], low), blk_swap(near[to ^ high][half:], high)]
            )
    far = {to: grp_swap(near[to], 1) for to in near}

    b = b3c.reshape(lam, BAND * BS, q)
    cols = min(2 * LANES, q)
    paired = [transform(b, virt, occ, cols, h) for h in range(q // cols)]

    slots, rows, count = schedule(codes, aux)
    owners = jnp.arange(n_blk, dtype=jnp.int32) ^ group
    pair = jnp.arange(KB * BAND, dtype=jnp.int32)
    nu = (owners[:, None] * KB + (pair // BAND + pair % BAND)[None, :]) % blocks
    chi = None
    for to in range(n_blk):
        chi = contract(
            near[to], far[to], paired, nu[to], slots[to], rows[to], count[to], aux, chi
        )
    chi = chi[:aux].reshape(n_blk, PBD * PB, q)

    total = lax.dynamic_index_in_dim(chi, group, 0, False)
    for d in range(1, n_blk):
        piece = lax.dynamic_index_in_dim(chi, group ^ d, 0, False)
        total = total + blk_swap(piece.astype(jnp.bfloat16), d).astype(jnp.float32)
    return total


def solution(mesh):
    in_specs = (
        P("blk", None, None, "grp"),
        P("blk", "grp"),
        P(None, "grp"),
        P(),
        P(("blk", "grp"), None, None),
        P(("blk", "grp")),
    )
    out_specs = P("blk", "grp")
    return jax.shard_map(local, mesh=mesh, in_specs=in_specs, out_specs=out_specs, check_vma=False)
```

```python
import functools

import jax
import jax.numpy as jnp
from jax import lax
from jax.experimental import pallas as pl
from jax.experimental.pallas import tpu as pltpu
from jax.sharding import PartitionSpec as P

BS = 32
PB = 32
KB = 3
BAND = 3
PBD = 4
LANES = 128
NU_PART = 6
SUB = 2


def transform_kernel(pitch, gv_ref, go_ref, b_ref, out_ref, *scratch):
    part, at_sub = pl.program_id(0), pl.program_id(1)
    rows = gv_ref.shape[1]
    lam = b_ref.shape[0]

    @pl.when(at_sub == 0)
    def _():
        for at in range(lam):
            r = jnp.dot(gv_ref[at // BS], b_ref[at], preferred_element_type=jnp.float32)
            for c, s in enumerate(scratch):
                s[pl.ds(at, rows, stride=pitch), :] = r[:, c * LANES : (c + 1) * LANES]

    for nb in range(SUB):
        here = at_sub * SUB + nb
        start = pl.multiple_of((part * (rows // BS) + here) * BS, BS)
        occ = go_ref[pl.ds(start, BAND * BS), :]
        zero = jnp.zeros_like(occ)
        occ = jnp.concatenate(
            [jnp.concatenate([occ, zero], axis=1), jnp.concatenate([zero, occ], axis=1)], axis=0
        )
        for i in range(BS // 2):
            at = (here * BS + 2 * i) * pitch
            w = jnp.concatenate(
                [
                    jnp.concatenate([s[pl.ds(at, lam), :], s[pl.ds(at + pitch, lam), :]], axis=0)
                    for s in scratch
                ],
                axis=1,
            )
            r = jnp.dot(occ, w.astype(jnp.bfloat16), preferred_element_type=jnp.float32)
            r = r.astype(jnp.bfloat16)
            for h in range(2):
                for j in range(BAND):
                    row = (h * BAND + j) * BS
                    to = (2 * i + h) * BS
                    out_ref[nb, BAND - 1 - j, to : to + BS, :] = r[row : row + BS]


def transform(b, gv, go, cols, which):
    lam, band, q = b.shape
    nb_total = gv.shape[1] // BS
    parts = nb_total // NU_PART
    rows = NU_PART * BS
    pitch = lam + 2
    subs = NU_PART // SUB
    return pl.pallas_call(
        functools.partial(transform_kernel, pitch),
        grid=(parts, subs),
        in_specs=[
            pl.BlockSpec((lam // BS, rows, band), lambda j, i: (0, j, 0)),
            pl.BlockSpec(go.shape, lambda j, i: (0, 0)),
            pl.BlockSpec((lam, band, cols), lambda j, i: (0, 0, which)),
        ],
        out_specs=pl.BlockSpec((SUB, BAND, BS * BS, cols), lambda j, i: (j * subs + i, 0, 0, 0)),
        out_shape=jax.ShapeDtypeStruct((nb_total, BAND, BS * BS, cols), jnp.bfloat16),
        scratch_shapes=[pltpu.VMEM((rows * pitch, LANES), jnp.float32)] * (cols // LANES),
        compiler_params=pltpu.CompilerParams(vmem_limit_bytes=62 * 2**20),
        cost_estimate=pl.CostEstimate(
            flops=150 * 10**8, bytes_accessed=24 * 2**20, transcendentals=0
        ),
        name="transform",
    )(gv, go, b)


def tiles_kernel(masks, halves, first, nu_ref, code_ref, *refs):
    groups = len(masks)
    near, far = refs[:groups], refs[groups : 2 * groups]
    paired = refs[2 * groups : 2 * groups + BAND * halves]
    out_ref, table, count = refs[-3:]
    aux = out_ref.shape[0] - 1
    pairs = KB * BAND
    slots = near[0].shape[0]
    step = pl.program_id(0)

    @pl.when(step == 0)
    def _():
        if first:
            out_ref[...] = jnp.zeros_like(out_ref)
        else:
            out_ref[...] = refs[-4][...]
        for at in range(groups * pairs * 2):
            count[at] = 0
        for g, mask in enumerate(masks):
            for side in range(2):

                def put(s, carry):
                    code = code_ref[(mask * 2 + side) * slots + s]

                    @pl.when(code >= 0)
                    def _():
                        at = (g * pairs + lax.rem(code, pairs)) * 2 + side
                        n = count[at]
                        table[at * slots + n] = lax.div(code, pairs) * slots + s
                        count[at] = n + 1

                    return carry

                lax.fori_loop(0, slots, put, 0)

    def item(g, d, i):
        pair = step * BAND + d
        rows, lhs = [], []
        for side, ref in ((0, near[g]), (1, far[g])):
            for n in (2 * i, 2 * i + 1):
                at = pair * 2 + side
                entry = jnp.where(n < count[at], table[at * slots + n], aux * slots)
                rows.append(lax.div(entry, slots))
                lhs.append(ref[lax.rem(entry, slots)])
        lhs = jnp.concatenate(lhs, axis=0)
        for h in range(halves):
            rhs = paired[d * halves + h]
            cols = rhs.shape[3]
            r = jnp.dot(lhs, rhs[0, 0], preferred_element_type=jnp.float32)
            for t in range(4):
                out_ref[rows[t], :, h * cols : (h + 1) * cols] += r[t * PB : (t + 1) * PB]

    for g in range(groups):

        @pl.when(step // KB == g)
        def _():
            for d in range(BAND):
                item(g, d, 0)
            for d in range(BAND):
                at = (step * BAND + d) * 2
                more = (jnp.maximum(count[at], count[at + 1]) + 1) // 2

                def again(i, carry):
                    item(g, d, i)
                    return carry

                lax.fori_loop(1, more, again, 0)


def contract(near, far, paired, nu, codes, aux, masks, total):
    halves = len(paired)
    cols = paired[0].shape[3]
    q = halves * cols
    groups, pairs = len(masks), KB * BAND
    slots = near[0].shape[0]
    first = total is None
    acc = pl.BlockSpec((aux + 1, PB, q), lambda m, *_: (0, 0, 0))
    whole = pl.BlockSpec(near[0].shape, lambda m, *_: (0, 0, 0))

    def paired_spec(d):
        def where(m, nu, *_):
            mask = sum(jnp.where(m // KB == g, masks[g], 0) for g in range(groups))
            return nu[mask * pairs + m % KB * BAND + d], d, 0, 0

        return pl.BlockSpec((1, 1, BS * BS, cols), where)

    return pl.pallas_call(
        functools.partial(tiles_kernel, masks, halves, first),
        grid_spec=pltpu.PrefetchScalarGridSpec(
            num_scalar_prefetch=2,
            grid=(KB * groups,),
            in_specs=[whole] * (2 * groups)
            + [paired_spec(d) for d in range(BAND) for _ in range(halves)]
            + ([] if first else [acc]),
            out_specs=acc,
            scratch_shapes=[
                pltpu.SMEM((groups * pairs * 2 * slots,), jnp.int32),
                pltpu.SMEM((groups * pairs * 2,), jnp.int32),
            ],
        ),
        out_shape=jax.ShapeDtypeStruct((aux + 1, PB, q), jnp.float32),
        compiler_params=pltpu.CompilerParams(vmem_limit_bytes=62 * 2**20),
        cost_estimate=pl.CostEstimate(
            flops=40 * 10**8 * groups, bytes_accessed=12 * 2**20 * groups, transcendentals=0
        ),
        name="contract",
    )(nu, codes, *near, *far, *(list(paired) * BAND), *([] if first else [total]))


def local(b3c, green_occ, green_virt, occ_mask, a_tiles, tile_codes):
    n_blk, n_grp = lax.axis_size("blk"), lax.axis_size("grp")
    group, member = lax.axis_index("blk"), lax.axis_index("grp")
    lam, _, _, q = b3c.shape
    basis, wide = green_virt.shape
    blocks = basis // BS
    aux = n_blk * PBD
    slots_here = a_tiles.shape[0]
    spread = n_grp // 2

    def grp_swap(a, bits):
        return lax.ppermute(a, "grp", [(i, i ^ bits) for i in range(n_grp)])

    def blk_swap(a, bits):
        return lax.ppermute(a, "blk", [(i, i ^ bits) for i in range(n_blk)])

    turned = a_tiles.reshape(slots_here, PB, BS, BS).swapaxes(2, 3).reshape(a_tiles.shape)

    coded = jnp.stack([tile_codes // (KB * BAND), tile_codes % (KB * BAND)])
    coded = jnp.where(tile_codes >= 0, coded, -1).astype(jnp.bfloat16)
    coded = jnp.pad(coded, ((0, 14), (0, wide - slots_here)))
    small = jnp.concatenate([green_virt, green_occ, coded], axis=0)[None]
    bit = 1
    while bit < n_grp:
        small = jnp.concatenate([small, grp_swap(small, bit)], axis=0)
        bit *= 2
    turned, small = lax.optimization_barrier((turned, small))
    ordered = jnp.take(small[:, : basis + lam], jnp.arange(n_grp, dtype=jnp.int32) ^ member, axis=0)
    virt_all = ordered[:, :basis].swapaxes(0, 1).reshape(basis, basis)
    occ_rows = ordered[:, basis:].swapaxes(0, 1).reshape(lam, basis)
    code_rows = -(-2 * n_grp * slots_here // (16 * lam)) * 16
    part = small[:, basis + lam : basis + lam + 2, :slots_here].swapaxes(0, 1).reshape(2, -1)
    part = jnp.pad(part, ((0, 0), (0, code_rows // 2 * lam - part.shape[1])))
    part = part.reshape(code_rows, lam)
    received = []
    for mask in range(n_blk):
        mine = lax.dynamic_slice_in_dim(occ_rows, (group ^ mask) * lam, lam, 1)
        packet = jnp.concatenate([mine, part], axis=0)
        received.append(blk_swap(packet, mask) if mask else packet)
    received = jnp.stack(received)
    occ = jnp.take(received[:, :lam], jnp.arange(n_blk, dtype=jnp.int32) ^ group, axis=0)
    occ = occ.reshape(basis, lam)
    part = received[:, lam:].reshape(n_blk, 2, -1)[:, :, : n_grp * slots_here].astype(jnp.int32)
    codes = jnp.where(part[:, 0] >= 0, part[:, 0] * (KB * BAND) + part[:, 1], -1)
    codes = codes.reshape(n_blk, spread, 2, slots_here).swapaxes(1, 2).reshape(-1)

    mask = lax.dynamic_slice_in_dim(occ_mask, group * KB, KB, 1)
    mask = jnp.repeat(jnp.repeat(mask, BS, axis=0), BS, axis=1).astype(jnp.bfloat16)
    occ = occ * mask
    occ = jnp.concatenate([occ[-(BAND - 1) * BS :], occ], axis=0)
    virt = jnp.concatenate([virt_all, virt_all[:, : (BAND - 1) * BS]], axis=1)
    virt = lax.dynamic_slice_in_dim(virt, group * lam, lam + (BAND - 1) * BS, 1)
    virt = jnp.stack([virt[:, l * BS : (l + BAND) * BS] for l in range(KB)])

    owners = jnp.arange(n_blk, dtype=jnp.int32) ^ group
    pair = jnp.arange(KB * BAND, dtype=jnp.int32)
    nu = ((owners[:, None] * KB + (pair // BAND + pair % BAND)[None, :]) % blocks).reshape(-1)

    b = b3c.reshape(lam, BAND * BS, q)
    cols = min(2 * LANES, q)
    hops = [grp_swap(turned, 2 * d) for d in range(1, spread)]
    paired = [transform(b, virt, occ, cols, 0)]
    hops, paired[0] = lax.optimization_barrier((hops, paired[0]))
    near = {0: jnp.concatenate([turned] + hops)}
    bits = [1 << i for i in range((n_blk - 1).bit_length())]
    for to in bits:
        near[to] = blk_swap(near[0], to)
    far = {0: grp_swap(near[0], 1)}
    paired += [transform(b, virt, occ, cols, h) for h in range(1, q // cols)]
    chi = contract([near[0]], [far[0]], paired, nu, codes, aux, (0,), None)
    levels = [[m for m in range(n_blk) if m.bit_count() == n] for n in range(1, len(bits) + 1)]
    arriving = [[near[to]] for to in bits]
    half = near[0].shape[0] // 2
    for masks, after in zip(levels, levels[1:] + [[]]):
        arriving, chi = lax.optimization_barrier((arriving, chi))
        for to, pieces in zip(masks, arriving):
            near[to] = pieces[0] if len(pieces) == 1 else jnp.concatenate(pieces)
        arriving = []
        for to in after:
            low, high = to & -to, 1 << (to.bit_length() - 1)
            arriving.append(
                [blk_swap(near[to ^ low][:half], low), blk_swap(near[to ^ high][half:], high)]
            )
        for to in masks:
            far[to] = grp_swap(near[to], 1)
        for at in range(0, len(masks), 2):
            now = tuple(masks[at : at + 2])
            chi = contract(
                [near[m] for m in now], [far[m] for m in now], paired, nu, codes, aux, now, chi
            )
    chi = chi[:aux].reshape(n_blk, PBD * PB, q)

    total = lax.dynamic_index_in_dim(chi, group, 0, False)
    for d in range(1, n_blk):
        piece = lax.dynamic_index_in_dim(chi, group ^ d, 0, False)
        total = total + blk_swap(piece.astype(jnp.bfloat16), d).astype(jnp.float32)
    return total


def solution(mesh):
    in_specs = (
        P("blk", None, None, "grp"),
        P("blk", "grp"),
        P(None, "grp"),
        P(),
        P(("blk", "grp"), None, None),
        P(("blk", "grp")),
    )
    out_specs = P("blk", "grp")
    return jax.shard_map(local, mesh=mesh, in_specs=in_specs, out_specs=out_specs, check_vma=False)
```

```python
import functools

import jax
import jax.numpy as jnp
from jax import lax
from jax.experimental import pallas as pl
from jax.experimental.pallas import tpu as pltpu
from jax.sharding import PartitionSpec as P


BS = 32
PB = 32
KB = 3
BAND = 3
PBD = 4
LANES = 128
NU_PART = 6
SUB = 2


def transform_kernel(pitch, begin, gv_ref, go_ref, b_ref, *refs):
    part, at_sub = pl.program_id(0) + begin, pl.program_id(1)
    halves = b_ref.shape[2] // LANES
    out_ref, scratch = refs[-1 - halves], refs[-halves:]
    rows = gv_ref.shape[1]
    lam = b_ref.shape[0]

    @pl.when(at_sub == 0)
    def _():
        for at in range(lam):
            r = jnp.dot(gv_ref[at // BS], b_ref[at], preferred_element_type=jnp.float32)
            for c, s in enumerate(scratch):
                s[pl.ds(at, rows, stride=pitch), :] = r[:, c * LANES : (c + 1) * LANES]

    for nb in range(SUB):
        here = at_sub * SUB + nb
        start = pl.multiple_of((part * (rows // BS) + here) * BS, BS)
        occ = go_ref[pl.ds(start, BAND * BS), :]
        zero = jnp.zeros_like(occ)
        occ = jnp.concatenate(
            [jnp.concatenate([occ, zero], axis=1), jnp.concatenate([zero, occ], axis=1)], axis=0
        )
        for i in range(BS // 2):
            at = (here * BS + 2 * i) * pitch
            w = jnp.concatenate(
                [
                    jnp.concatenate([s[pl.ds(at, lam), :], s[pl.ds(at + pitch, lam), :]], axis=0)
                    for s in scratch
                ],
                axis=1,
            )
            r = jnp.dot(occ, w.astype(jnp.bfloat16), preferred_element_type=jnp.float32)
            r = r.astype(jnp.bfloat16)
            for h in range(2):
                for j in range(BAND):
                    row = (h * BAND + j) * BS
                    to = (2 * i + h) * BS
                    out_ref[nb, BAND - 1 - j, to : to + BS, :] = r[row : row + BS]


def transform(b, gv, go, cols, which, begin, end, into=None):
    lam, band, _ = b.shape
    nb_total = gv.shape[1] // BS
    rows = NU_PART * BS
    pitch = lam + 2
    subs = NU_PART // SUB
    held = [] if into is None else [into]
    return pl.pallas_call(
        functools.partial(transform_kernel, pitch, begin),
        grid=(end - begin, subs),
        in_specs=[
            pl.BlockSpec((lam // BS, rows, band), lambda j, i: (0, j + begin, 0)),
            pl.BlockSpec(go.shape, lambda j, i: (0, 0)),
            pl.BlockSpec((lam, band, cols), lambda j, i: (0, 0, which)),
        ]
        + [pl.BlockSpec(memory_space=pl.ANY)] * len(held),
        out_specs=pl.BlockSpec(
            (SUB, BAND, BS * BS, cols), lambda j, i: ((j + begin) * subs + i, 0, 0, 0)
        ),
        out_shape=jax.ShapeDtypeStruct((nb_total, BAND, BS * BS, cols), jnp.bfloat16),
        scratch_shapes=[pltpu.VMEM((rows * pitch, LANES), jnp.float32)] * (cols // LANES),
        input_output_aliases={3: 0} if held else {},
        compiler_params=pltpu.CompilerParams(vmem_limit_bytes=62 * 2**20),
        cost_estimate=pl.CostEstimate(
            flops=75 * 10**8 * (end - begin), bytes_accessed=12 * 2**20, transcendentals=0
        ),
        name="transform",
    )(gv, go, b, *held)


def tiles_kernel(masks, halves, nu_ref, code_ref, *refs):
    groups, pairs = len(masks), KB * BAND
    sources, paired = refs[: 2 * groups], refs[2 * groups : 2 * groups + halves]
    out_ref, tiles, rhs, table, count, tile_sem, pair_sem = refs[-7:]
    aux = out_ref.shape[0] - 1
    slots = tiles.shape[2]
    cols = rhs.shape[3]

    def tile_copy(g, side):
        return pltpu.make_async_copy(sources[2 * g + side], tiles.at[g, side], tile_sem.at[g, side])

    def pair_copy(mask, at, p, h):
        return pltpu.make_async_copy(
            paired[h].at[nu_ref[mask * pairs + p], p % BAND], rhs.at[at, h], pair_sem.at[at, h]
        )

    for g, mask in enumerate(masks):
        for side in range(2):
            tile_copy(g, side).start()
        for p in range(pairs):
            for h in range(halves):
                pair_copy(mask, g * pairs + p, p, h).start()
    out_ref[...] = jnp.zeros_like(out_ref)
    for at in range(groups * pairs * 2):
        count[at] = 0
    for g, mask in enumerate(masks):
        for side in range(2):

            def put(s, carry):
                code = code_ref[(mask * 2 + side) * slots + s]

                @pl.when(code >= 0)
                def _():
                    at = (g * pairs + lax.rem(code, pairs)) * 2 + side
                    n = count[at]
                    table[at * slots + n] = lax.div(code, pairs) * 256 + s
                    count[at] = n + 1

                return carry

            lax.fori_loop(0, slots, put, 0)

    def item(g, pair, i):
        rows, lhs = [], []
        for side in range(2):
            for n in (2 * i, 2 * i + 1):
                at = pair * 2 + side
                entry = jnp.where(n < count[at], table[at * slots + n], aux * 256)
                rows.append(entry >> 8)
                lhs.append(tiles[g, side, entry & 255])
        lhs = jnp.concatenate(lhs, axis=0)
        for h in range(halves):
            r = jnp.dot(lhs, rhs[pair, h], preferred_element_type=jnp.float32)
            for t in range(4):
                out_ref[rows[t], :, h * cols : (h + 1) * cols] += r[t * PB : (t + 1) * PB]

    for g, mask in enumerate(masks):
        for side in range(2):
            tile_copy(g, side).wait()
        for p in range(pairs):
            for h in range(halves):
                pair_copy(mask, g * pairs + p, p, h).wait()
        for p in range(pairs):
            item(g, g * pairs + p, 0)

    def rest(pair, carry):
        more = (jnp.maximum(count[2 * pair], count[2 * pair + 1]) + 1) // 2

        def again(i, carry):
            item(pair // pairs, pair, i)
            return carry

        return lax.fori_loop(1, more, again, carry)

    lax.fori_loop(0, groups * pairs, rest, 0)


def contract(near, far, paired, nu, codes, aux, masks):
    halves = len(paired)
    cols = paired[0].shape[3]
    q = halves * cols
    groups, pairs = len(masks), KB * BAND
    slots = near[0].shape[0]
    acc = pl.BlockSpec((aux + 1, PB, q), lambda i, *_: (0, 0, 0))
    far_memory = pl.BlockSpec(memory_space=pltpu.HBM)
    return pl.pallas_call(
        functools.partial(tiles_kernel, masks, halves),
        grid_spec=pltpu.PrefetchScalarGridSpec(
            num_scalar_prefetch=2,
            grid=(1,),
            in_specs=[far_memory] * (2 * groups + halves),
            out_specs=acc,
            scratch_shapes=[
                pltpu.VMEM((groups, 2) + near[0].shape, jnp.bfloat16),
                pltpu.VMEM((groups * pairs, halves, BS * BS, cols), jnp.bfloat16),
                pltpu.SMEM((groups * pairs * 2 * slots,), jnp.int32),
                pltpu.SMEM((groups * pairs * 2,), jnp.int32),
                pltpu.SemaphoreType.DMA((groups, 2)),
                pltpu.SemaphoreType.DMA((groups * pairs, halves)),
            ],
        ),
        out_shape=jax.ShapeDtypeStruct((aux + 1, PB, q), jnp.float32),
        compiler_params=pltpu.CompilerParams(vmem_limit_bytes=62 * 2**20),
        cost_estimate=pl.CostEstimate(
            flops=40 * 10**8 * groups, bytes_accessed=12 * 2**20 * groups, transcendentals=0
        ),
        name="contract",
    )(
        nu,
        codes,
        *[side for pair in zip(near, far) for side in pair],
        *paired,
    )


def local(b3c, green_occ, green_virt, occ_mask, a_tiles, tile_codes):
    n_blk, n_grp = lax.axis_size("blk"), lax.axis_size("grp")
    group, member = lax.axis_index("blk"), lax.axis_index("grp")
    lam, _, _, q = b3c.shape
    basis, wide = green_virt.shape
    blocks = basis // BS
    aux = n_blk * PBD
    slots_here = a_tiles.shape[0]
    spread = n_grp // 2

    def grp_swap(a, bits):
        return lax.ppermute(a, "grp", [(i, i ^ bits) for i in range(n_grp)])

    def blk_swap(a, bits):
        return lax.ppermute(a, "blk", [(i, i ^ bits) for i in range(n_blk)])

    turned = a_tiles.reshape(slots_here, PB, BS, BS).swapaxes(2, 3).reshape(a_tiles.shape)

    coded = jnp.stack([tile_codes // (KB * BAND), tile_codes % (KB * BAND)])
    coded = jnp.where(tile_codes >= 0, coded, -1).astype(jnp.bfloat16)
    coded = jnp.pad(coded, ((0, 14), (0, wide - slots_here)))
    small = jnp.concatenate([green_virt, green_occ, coded], axis=0)[None]
    bit = 2
    while bit < n_grp:
        moved = grp_swap(small, bit)
        small = jnp.concatenate([small, moved], axis=0)
        bit *= 2
    small = jnp.concatenate([small, grp_swap(small, 1)], axis=0)
    relative = jnp.arange(n_grp, dtype=jnp.int32) ^ member
    order = relative % 2 * spread + relative // 2
    ordered = jnp.take(small[:, : basis + lam], order, axis=0)
    virt_all = ordered[:, :basis].swapaxes(0, 1).reshape(basis, basis)
    occ_rows = ordered[:, basis:].swapaxes(0, 1).reshape(lam, basis)
    code_rows = -(-2 * n_grp * slots_here // (16 * lam)) * 16
    part = small[:, basis + lam : basis + lam + 2, :slots_here].swapaxes(0, 1).reshape(2, -1)
    part = jnp.pad(part, ((0, 0), (0, code_rows // 2 * lam - part.shape[1])))
    part = part.reshape(code_rows, lam)
    received = []
    for mask in range(n_blk):
        mine = lax.dynamic_slice_in_dim(occ_rows, (group ^ mask) * lam, lam, 1)
        packet = jnp.concatenate([mine, part], axis=0)
        received.append(blk_swap(packet, mask) if mask else packet)
    received = jnp.stack(received)
    occ = jnp.take(received[:, :lam], jnp.arange(n_blk, dtype=jnp.int32) ^ group, axis=0)
    occ = occ.reshape(basis, lam)
    part = received[:, lam:].reshape(n_blk, 2, -1)[:, :, : n_grp * slots_here].astype(jnp.int32)
    codes = jnp.where(part[:, 0] >= 0, part[:, 0] * (KB * BAND) + part[:, 1], -1)
    codes = codes.reshape(-1)

    mask = lax.dynamic_slice_in_dim(occ_mask, group * KB, KB, 1)
    mask = jnp.repeat(jnp.repeat(mask, BS, axis=0), BS, axis=1).astype(jnp.bfloat16)
    occ = occ * mask
    occ = jnp.concatenate([occ[-(BAND - 1) * BS :], occ], axis=0)
    virt = jnp.concatenate([virt_all, virt_all[:, : (BAND - 1) * BS]], axis=1)
    virt = lax.dynamic_slice_in_dim(virt, group * lam, lam + (BAND - 1) * BS, 1)
    virt = jnp.stack([virt[:, l * BS : (l + BAND) * BS] for l in range(KB)])

    owners = jnp.arange(n_blk, dtype=jnp.int32) ^ group
    pair = jnp.arange(KB * BAND, dtype=jnp.int32)
    nu = ((owners[:, None] * KB + (pair // BAND + pair % BAND)[None, :]) % blocks).reshape(-1)

    b = b3c.reshape(lam, BAND * BS, q)
    cols = min(2 * LANES, q)
    parts = blocks // NU_PART
    hops = []
    for d in range(1, spread):
        hops.append(grp_swap(turned, 2 * d))
    paired = transform(b, virt, occ, cols, 0, 0, 1)
    hops, paired = lax.optimization_barrier((hops, paired))
    near = {0: jnp.concatenate([turned] + hops)}
    bits = [1 << i for i in range((n_blk - 1).bit_length())]
    for to in bits:
        near[to] = blk_swap(near[0], to)
    far = {0: grp_swap(near[0], 1)}
    paired = [transform(b, virt, occ, cols, 0, 1, parts, paired)]
    paired += [transform(b, virt, occ, cols, h, 0, parts) for h in range(1, q // cols)]
    arriving, paired = lax.optimization_barrier(([[near[to]] for to in bits], paired))
    levels = [[m for m in range(n_blk) if m.bit_count() == n] for n in range(1, len(bits) + 1)]
    half = near[0].shape[0] // 2
    sums, first = [], [0]
    for masks, after in zip(levels, levels[1:] + [[]]):
        for to, pieces in zip(masks, arriving):
            near[to] = pieces[0] if len(pieces) == 1 else jnp.concatenate(pieces)
        arriving = []
        for to in after:
            low, high = to & -to, 1 << (to.bit_length() - 1)
            arriving.append(
                [blk_swap(near[to ^ low][:half], low), blk_swap(near[to ^ high][half:], high)]
            )
        for to in masks:
            far[to] = grp_swap(near[to], 1)
        now = tuple(first + masks)
        first = []
        chi = contract([near[m] for m in now], [far[m] for m in now], paired, nu, codes, aux, now)
        arriving, chi = lax.optimization_barrier((arriving, chi))
        sums.append(chi[:aux].reshape(n_blk, PBD * PB, q))

    def piece(d):
        return sum(lax.dynamic_index_in_dim(chi, group ^ d, 0, False) for chi in sums)

    total = piece(0)
    for d in range(1, n_blk):
        total = total + blk_swap(piece(d).astype(jnp.bfloat16), d).astype(jnp.float32)
    return total


def solution(mesh):
    in_specs = (
        P("blk", None, None, "grp"),
        P("blk", "grp"),
        P(None, "grp"),
        P(),
        P(("blk", "grp"), None, None),
        P(("blk", "grp")),
    )
    out_specs = P("blk", "grp")
    return jax.shard_map(local, mesh=mesh, in_specs=in_specs, out_specs=out_specs, check_vma=False)
```

```python
import functools

import jax
import jax.numpy as jnp
from jax import lax
from jax.experimental import pallas as pl
from jax.experimental.pallas import tpu as pltpu
from jax.sharding import PartitionSpec as P


BS = 32
PB = 32
KB = 3
BAND = 3
PBD = 4
LANES = 128
NU_PART = 6
SUB = 2


def transform_kernel(pitch, gv_ref, go_ref, b_ref, out_ref, *scratch):
    part, at_sub = pl.program_id(0), pl.program_id(1)
    rows = gv_ref.shape[1]
    lam = b_ref.shape[0]

    @pl.when(at_sub == 0)
    def _():
        for at in range(lam):
            r = jnp.dot(gv_ref[at // BS], b_ref[at], preferred_element_type=jnp.float32)
            for c, s in enumerate(scratch):
                s[pl.ds(at, rows, stride=pitch), :] = r[:, c * LANES : (c + 1) * LANES]

    for nb in range(SUB):
        here = at_sub * SUB + nb
        start = pl.multiple_of((part * (rows // BS) + here) * BS, BS)
        occ = go_ref[pl.ds(start, BAND * BS), :]
        zero = jnp.zeros_like(occ)
        occ = jnp.concatenate(
            [jnp.concatenate([occ, zero], axis=1), jnp.concatenate([zero, occ], axis=1)], axis=0
        )
        for i in range(BS // 2):
            at = (here * BS + 2 * i) * pitch
            w = jnp.concatenate(
                [
                    jnp.concatenate([s[pl.ds(at, lam), :], s[pl.ds(at + pitch, lam), :]], axis=0)
                    for s in scratch
                ],
                axis=1,
            )
            r = jnp.dot(occ, w.astype(jnp.bfloat16), preferred_element_type=jnp.float32)
            r = r.astype(jnp.bfloat16)
            for h in range(2):
                for j in range(BAND):
                    row = (h * BAND + j) * BS
                    to = (2 * i + h) * BS
                    out_ref[nb, BAND - 1 - j, to : to + BS, :] = r[row : row + BS]


def transform(b, gv, go, cols, which):
    lam, band, _ = b.shape
    nb_total = gv.shape[1] // BS
    rows = NU_PART * BS
    pitch = lam + 2
    subs = NU_PART // SUB
    parts = nb_total // NU_PART
    return pl.pallas_call(
        functools.partial(transform_kernel, pitch),
        grid=(parts, subs),
        in_specs=[
            pl.BlockSpec((lam // BS, rows, band), lambda j, i: (0, j, 0)),
            pl.BlockSpec(go.shape, lambda j, i: (0, 0)),
            pl.BlockSpec((lam, band, cols), lambda j, i: (0, 0, which)),
        ],
        out_specs=pl.BlockSpec(
            (SUB, BAND, BS * BS, cols), lambda j, i: (j * subs + i, 0, 0, 0)
        ),
        out_shape=jax.ShapeDtypeStruct((nb_total, BAND, BS * BS, cols), jnp.bfloat16),
        scratch_shapes=[pltpu.VMEM((rows * pitch, LANES), jnp.float32)] * (cols // LANES),
        compiler_params=pltpu.CompilerParams(vmem_limit_bytes=62 * 2**20),
        cost_estimate=pl.CostEstimate(
            flops=75 * 10**8 * parts, bytes_accessed=12 * 2**20, transcendentals=0
        ),
        name="transform",
    )(gv, go, b)


def tiles_kernel(masks, halves, code_ref, *refs):
    groups, pairs = len(masks), KB * BAND
    sources, paired = refs[: 2 * groups], refs[2 * groups : 2 * groups + halves]
    out_ref, tiles, rhs, table, count, jobs, tile_sem, pair_sem = refs[-8:]
    aux = out_ref.shape[0] - 1
    slots = tiles.shape[2]
    cols = rhs.shape[3]
    group = lax.axis_index("blk")
    blocks = paired[0].shape[0]

    def tile_copy(g, side):
        return pltpu.make_async_copy(sources[2 * g + side], tiles.at[g, side], tile_sem.at[g, side])

    def pair_copy(mask, at, p, h):
        nu = lax.rem((group ^ mask) * KB + p // BAND + p % BAND, blocks)
        return pltpu.make_async_copy(
            paired[h].at[nu, p % BAND], rhs.at[at, h], pair_sem.at[at, h]
        )

    for g, mask in enumerate(masks):
        for side in range(2):
            tile_copy(g, side).start()
        for p in range(pairs):
            for h in range(halves):
                pair_copy(mask, g * pairs + p, p, h).start()
    out_ref[...] = jnp.zeros_like(out_ref)
    for at in range(groups * pairs * 2):
        count[at] = 0
    jobs[0] = 0
    for g, mask in enumerate(masks):
        for side in range(2):

            def put(s, carry):
                code = code_ref[(mask * 2 + side) * slots + s]

                @pl.when(code >= 0)
                def _():
                    at = (g * pairs + lax.rem(code, pairs)) * 2 + side
                    n = count[at]
                    table[at * slots + n] = lax.div(code, pairs) * 256 + s
                    count[at] = n + 1

                    @pl.when((n > 1) & (n % 2 == 0) & ((side == 0) | (count[at - side] <= n)))
                    def _():
                        jobs[0] = jobs[0] + 1
                        jobs[jobs[0]] = at // 2 * 256 + n // 2

                return carry

            lax.fori_loop(0, slots, put, 0)

    def item(g, pair, i):
        rows, lhs = [], []
        for side in range(2):
            for n in (2 * i, 2 * i + 1):
                at = pair * 2 + side
                entry = jnp.where(n < count[at], table[at * slots + n], aux * 256)
                rows.append(entry >> 8)
                lhs.append(tiles[g, side, entry & 255])
        lhs = jnp.concatenate(lhs, axis=0)
        for h in range(halves):
            r = jnp.dot(lhs, rhs[pair, h], preferred_element_type=jnp.float32)
            for t in range(4):
                out_ref[rows[t], :, h * cols : (h + 1) * cols] += r[t * PB : (t + 1) * PB]

    for g, mask in enumerate(masks):
        for side in range(2):
            tile_copy(g, side).wait()
        for p in range(pairs):
            for h in range(halves):
                pair_copy(mask, g * pairs + p, p, h).wait()
        for p in range(pairs):
            item(g, g * pairs + p, 0)

    def again(job, carry):
        pair = jobs[job] >> 8
        item(lax.div(pair, pairs), pair, jobs[job] & 255)
        return carry

    lax.fori_loop(1, jobs[0] + 1, again, 0)


def contract(near, far, paired, codes, aux, masks):
    halves = len(paired)
    cols = paired[0].shape[3]
    q = halves * cols
    groups, pairs = len(masks), KB * BAND
    slots = near[0].shape[0]
    acc = pl.BlockSpec((aux + 1, PB, q), lambda i, *_: (0, 0, 0))
    far_memory = pl.BlockSpec(memory_space=pltpu.HBM)
    return pl.pallas_call(
        functools.partial(tiles_kernel, masks, halves),
        grid_spec=pltpu.PrefetchScalarGridSpec(
            num_scalar_prefetch=1,
            grid=(1,),
            in_specs=[far_memory] * (2 * groups + halves),
            out_specs=acc,
            scratch_shapes=[
                pltpu.VMEM((groups, 2) + near[0].shape, jnp.bfloat16),
                pltpu.VMEM((groups * pairs, halves, BS * BS, cols), jnp.bfloat16),
                pltpu.SMEM((groups * pairs * 2 * slots,), jnp.int32),
                pltpu.SMEM((groups * pairs * 2,), jnp.int32),
                pltpu.SMEM((groups * slots + 1,), jnp.int32),
                pltpu.SemaphoreType.DMA((groups, 2)),
                pltpu.SemaphoreType.DMA((groups * pairs, halves)),
            ],
        ),
        out_shape=jax.ShapeDtypeStruct((aux + 1, PB, q), jnp.float32),
        compiler_params=pltpu.CompilerParams(vmem_limit_bytes=62 * 2**20),
        cost_estimate=pl.CostEstimate(
            flops=40 * 10**8 * groups, bytes_accessed=12 * 2**20 * groups, transcendentals=0
        ),
        name="contract",
    )(
        codes,
        *[side for pair in zip(near, far) for side in pair],
        *paired,
    )


def local(b3c, green_occ, green_virt, occ_mask, a_tiles, tile_codes):
    n_blk, n_grp = lax.axis_size("blk"), lax.axis_size("grp")
    group, member = lax.axis_index("blk"), lax.axis_index("grp")
    lam, _, _, q = b3c.shape
    basis, wide = green_virt.shape
    aux = n_blk * PBD
    slots_here = a_tiles.shape[0]
    spread = n_grp // 2

    def grp_swap(a, bits):
        return lax.ppermute(a, "grp", [(i, i ^ bits) for i in range(n_grp)])

    def blk_swap(a, bits):
        return lax.ppermute(a, "blk", [(i, i ^ bits) for i in range(n_blk)])

    turned = a_tiles.reshape(slots_here, PB, BS, BS).swapaxes(2, 3).reshape(a_tiles.shape)

    per = n_grp // n_blk
    turn = [
        (k * n_grp + j, j // per * n_grp + k * per + j % per)
        for k in range(n_blk)
        for j in range(n_grp)
    ]
    occ_here = lax.ppermute(green_occ, ("blk", "grp"), turn)
    coded = jnp.stack([tile_codes >> 4, tile_codes & 15]).astype(jnp.bfloat16)
    coded = jnp.pad(coded, ((0, 14), (0, wide - slots_here)))
    coded = [coded if mask == 0 else blk_swap(coded, mask) for mask in range(n_blk)]
    coded = jnp.concatenate([c[:2] for c in coded], axis=0)
    coded = jnp.pad(coded, ((0, -coded.shape[0] % 16), (0, 0)))
    small = jnp.concatenate([green_virt, occ_here, coded], axis=0)[None]
    bit = 2
    while bit < n_grp:
        moved = grp_swap(small, bit)
        small = jnp.concatenate([small, moved], axis=0)
        bit *= 2
    small = jnp.concatenate([small, grp_swap(small, 1)], axis=0)
    relative = jnp.arange(n_grp, dtype=jnp.int32) ^ member
    order = relative % 2 * spread + relative // 2
    ordered = jnp.take(small[:, : basis + lam], order, axis=0)
    virt_all = ordered[:, :basis].swapaxes(0, 1).reshape(basis, basis)
    occ = ordered[:, basis:].reshape(n_blk, per, lam, wide).swapaxes(1, 2).reshape(basis, lam)
    part = small[:, basis + lam : basis + lam + 2 * n_blk, :slots_here].astype(jnp.int32)
    part = part.reshape(n_grp, n_blk, 2, slots_here)
    codes = (part[:, :, 0] * 16 + part[:, :, 1]).swapaxes(0, 1).reshape(-1)

    mask = lax.dynamic_slice_in_dim(occ_mask, group * KB, KB, 1)
    mask = jnp.repeat(jnp.repeat(mask, BS, axis=0), BS, axis=1).astype(jnp.bfloat16)
    occ = occ * mask
    occ = jnp.concatenate([occ[-(BAND - 1) * BS :], occ], axis=0)
    virt = jnp.concatenate([virt_all, virt_all[:, : (BAND - 1) * BS]], axis=1)
    virt = lax.dynamic_slice_in_dim(virt, group * lam, lam + (BAND - 1) * BS, 1)
    virt = jnp.stack([virt[:, l * BS : (l + BAND) * BS] for l in range(KB)])

    b = b3c.reshape(lam, BAND * BS, q)
    cols = min(2 * LANES, q)
    hops = []
    for d in range(1, spread):
        hops.append(grp_swap(turned, 2 * d))
    paired = [transform(b, virt, occ, cols, 0)]
    hops, paired = lax.optimization_barrier((hops, paired))
    near = {0: jnp.concatenate([turned] + hops)}
    bits = [1 << i for i in range((n_blk - 1).bit_length())]
    for to in bits:
        near[to] = blk_swap(near[0], to)
    far = {0: grp_swap(near[0], 1)}
    paired += [transform(b, virt, occ, cols, h) for h in range(1, q // cols)]
    chi = contract([near[0]], [far[0]], paired, codes, aux, (0,))
    arriving, chi = lax.optimization_barrier(([[near[to]] for to in bits], chi))
    sums = [chi]
    levels = [[m for m in range(n_blk) if m.bit_count() == n] for n in range(1, len(bits) + 1)]
    half = near[0].shape[0] // 2
    for masks, after in zip(levels, levels[1:] + [[]]):
        for to, pieces in zip(masks, arriving):
            near[to] = pieces[0] if len(pieces) == 1 else jnp.concatenate(pieces)
        arriving = []
        for to in after:
            low, high = to & -to, 1 << (to.bit_length() - 1)
            arriving.append(
                [blk_swap(near[to ^ low][:half], low), blk_swap(near[to ^ high][half:], high)]
            )
        for to in masks:
            far[to] = grp_swap(near[to], 1)
        chi = contract([near[m] for m in masks], [far[m] for m in masks], paired, codes, aux, masks)
        arriving, chi = lax.optimization_barrier((arriving, chi))
        sums.append(chi)

    def piece(d):
        rows = [lax.dynamic_slice_in_dim(chi, (group ^ d) * PBD, PBD, 0) for chi in sums]
        return sum(rows).reshape(PBD * PB, q)

    total = piece(0)
    for d in range(1, n_blk):
        total = total + blk_swap(piece(d).astype(jnp.bfloat16), d).astype(jnp.float32)
    return total


def solution(mesh):
    in_specs = (
        P("blk", None, None, "grp"),
        P("blk", "grp"),
        P(None, "grp"),
        P(),
        P(("blk", "grp"), None, None),
        P(("blk", "grp")),
    )
    out_specs = P("blk", "grp")
    return jax.shard_map(local, mesh=mesh, in_specs=in_specs, out_specs=out_specs, check_vma=False)
```

```python
import functools

import jax
import jax.numpy as jnp
from jax import lax
from jax.experimental import pallas as pl
from jax.experimental.pallas import tpu as pltpu
from jax.sharding import PartitionSpec as P

BS = 32
PB = 32
KB = 3
BAND = 3
PBD = 4
LANES = 128
NU_PART = 6
SUB = 2


def transform_kernel(pitch, gv_ref, go_ref, b_ref, out_ref, *scratch):
    part, at_sub = pl.program_id(0), pl.program_id(1)
    rows = gv_ref.shape[1]
    lam = b_ref.shape[0]

    @pl.when(at_sub == 0)
    def _():
        for at in range(lam):
            r = jnp.dot(gv_ref[at // BS], b_ref[at], preferred_element_type=jnp.float32)
            for c, s in enumerate(scratch):
                s[pl.ds(at, rows, stride=pitch), :] = r[:, c * LANES : (c + 1) * LANES]

    for nb in range(SUB):
        here = at_sub * SUB + nb
        start = pl.multiple_of((part * (rows // BS) + here) * BS, BS)
        occ = go_ref[pl.ds(start, BAND * BS), :]
        zero = jnp.zeros_like(occ)
        occ = jnp.concatenate(
            [jnp.concatenate([occ, zero], axis=1), jnp.concatenate([zero, occ], axis=1)], axis=0
        )
        for i in range(BS // 2):
            at = (here * BS + 2 * i) * pitch
            w = jnp.concatenate(
                [
                    jnp.concatenate([s[pl.ds(at, lam), :], s[pl.ds(at + pitch, lam), :]], axis=0)
                    for s in scratch
                ],
                axis=1,
            )
            r = jnp.dot(occ, w.astype(jnp.bfloat16), preferred_element_type=jnp.float32)
            r = r.astype(jnp.bfloat16)
            for h in range(2):
                for j in range(BAND):
                    row = (h * BAND + j) * BS
                    to = (2 * i + h) * BS
                    out_ref[nb, BAND - 1 - j, to : to + BS, :] = r[row : row + BS]


def transform(b, gv, go, cols, which):
    lam, band, q = b.shape
    nb_total = gv.shape[1] // BS
    rows = NU_PART * BS
    pitch = lam + 2
    subs = NU_PART // SUB
    parts = nb_total // NU_PART
    return pl.pallas_call(
        functools.partial(transform_kernel, pitch),
        grid=(parts, subs),
        in_specs=[
            pl.BlockSpec((lam // BS, rows, band), lambda j, i: (0, j, 0)),
            pl.BlockSpec(go.shape, lambda j, i: (0, 0)),
            pl.BlockSpec((lam, band, cols), lambda j, i: (0, 0, which)),
        ],
        out_specs=pl.BlockSpec(
            (SUB, BAND, BS * BS, cols), lambda j, i: (j * subs + i, 0, 0, 0)
        ),
        out_shape=jax.ShapeDtypeStruct((nb_total, BAND, BS * BS, cols), jnp.bfloat16),
        scratch_shapes=[pltpu.VMEM((rows * pitch, LANES), jnp.float32)] * (cols // LANES),
        compiler_params=pltpu.CompilerParams(vmem_limit_bytes=62 * 2**20),
        cost_estimate=pl.CostEstimate(
            flops=75 * 10**8 * parts, bytes_accessed=12 * 2**20, transcendentals=0
        ),
        name="transform",
    )(gv, go, b)


def tiles_kernel(masks, halves, wide, here, code_ref, *refs):
    groups, pairs = len(masks), KB * BAND
    sources, paired = refs[: 2 * groups], refs[2 * groups : 2 * groups + halves]
    out_ref, tiles, rhs, table, count, jobs, tile_sem, pair_sem = refs[-8:]
    aux = out_ref.shape[0] - 1
    slots = tiles.shape[2]
    cols = rhs.shape[3]
    group, member = lax.axis_index("blk"), lax.axis_index("grp")
    blocks = paired[0].shape[0]

    def tile_copy(g, side):
        return pltpu.make_async_copy(sources[2 * g + side], tiles.at[g, side], tile_sem.at[g, side])

    def pair_copy(mask, at, p, h):
        nu = lax.rem((group ^ mask) * KB + p // BAND + p % BAND, blocks)
        return pltpu.make_async_copy(
            paired[h].at[nu, p % BAND], rhs.at[at, h], pair_sem.at[at, h]
        )

    for g, mask in enumerate(masks):
        for side in range(2):
            tile_copy(g, side).start()
        for p in range(pairs):
            for h in range(halves):
                pair_copy(mask, g * pairs + p, p, h).start()
    out_ref[...] = jnp.zeros_like(out_ref)
    for at in range(groups * pairs * 2):
        count[at] = 0
    jobs[0] = 0
    for g, mask in enumerate(masks):
        for side in range(2):

            def put(s, carry):
                sender = member ^ (lax.div(s, here) * 2 + side)
                code = code_ref[mask * (blocks * BS) + sender * wide + lax.rem(s, here)]

                @pl.when(code >= 0)
                def _():
                    at = (g * pairs + lax.rem(code, pairs)) * 2 + side
                    n = count[at]
                    table[at * slots + n] = lax.div(code, pairs) * 256 + s
                    count[at] = n + 1

                    @pl.when((n > 1) & (n % 2 == 0) & ((side == 0) | (count[at - side] <= n)))
                    def _():
                        jobs[0] = jobs[0] + 1
                        jobs[jobs[0]] = at // 2 * 256 + n // 2

                return carry

            lax.fori_loop(0, slots, put, 0)

    def item(g, pair, i):
        rows, lhs = [], []
        for side in range(2):
            for n in (2 * i, 2 * i + 1):
                at = pair * 2 + side
                entry = jnp.where(n < count[at], table[at * slots + n], aux * 256)
                rows.append(entry >> 8)
                lhs.append(tiles[g, side, entry & 255])
        lhs = jnp.concatenate(lhs, axis=0)
        for h in range(halves):
            r = jnp.dot(lhs, rhs[pair, h], preferred_element_type=jnp.float32)
            for t in range(4):
                out_ref[rows[t], :, h * cols : (h + 1) * cols] += r[t * PB : (t + 1) * PB]

    for g, mask in enumerate(masks):
        for side in range(2):
            tile_copy(g, side).wait()
        for p in range(pairs):
            for h in range(halves):
                pair_copy(mask, g * pairs + p, p, h).wait()
        for p in range(pairs):
            item(g, g * pairs + p, 0)

    def again(job, carry):
        pair = jobs[job] >> 8
        item(lax.div(pair, pairs), pair, jobs[job] & 255)
        return carry

    lax.fori_loop(1, jobs[0] + 1, again, 0)


def contract(near, far, paired, codes, wide, here, aux, masks):
    halves = len(paired)
    cols = paired[0].shape[3]
    q = halves * cols
    groups, pairs = len(masks), KB * BAND
    slots = near[0].shape[0]
    acc = pl.BlockSpec((aux + 1, PB, q), lambda i, *_: (0, 0, 0))
    far_memory = pl.BlockSpec(memory_space=pltpu.HBM)
    return pl.pallas_call(
        functools.partial(tiles_kernel, masks, halves, wide, here),
        grid_spec=pltpu.PrefetchScalarGridSpec(
            num_scalar_prefetch=1,
            grid=(1,),
            in_specs=[far_memory] * (2 * groups + halves),
            out_specs=acc,
            scratch_shapes=[
                pltpu.VMEM((groups, 2) + near[0].shape, jnp.bfloat16),
                pltpu.VMEM((groups * pairs, halves, BS * BS, cols), jnp.bfloat16),
                pltpu.SMEM((groups * pairs * 2 * slots,), jnp.int32),
                pltpu.SMEM((groups * pairs * 2,), jnp.int32),
                pltpu.SMEM((groups * slots + 1,), jnp.int32),
                pltpu.SemaphoreType.DMA((groups, 2)),
                pltpu.SemaphoreType.DMA((groups * pairs, halves)),
            ],
        ),
        out_shape=jax.ShapeDtypeStruct((aux + 1, PB, q), jnp.float32),
        compiler_params=pltpu.CompilerParams(vmem_limit_bytes=62 * 2**20),
        cost_estimate=pl.CostEstimate(
            flops=40 * 10**8 * groups, bytes_accessed=12 * 2**20 * groups, transcendentals=0
        ),
        name="contract",
    )(
        codes,
        *[side for pair in zip(near, far) for side in pair],
        *paired,
    )


def local(b3c, green_occ, green_virt, occ_mask, a_tiles, tile_codes):
    n_blk, n_grp = lax.axis_size("blk"), lax.axis_size("grp")
    group = lax.axis_index("blk")
    lam, _, _, q = b3c.shape
    basis, wide = green_virt.shape
    blocks = basis // BS
    aux = n_blk * PBD
    slots_here = a_tiles.shape[0]
    spread = n_grp // 2

    def grp_swap(a, bits):
        return lax.ppermute(a, "grp", [(i, i ^ bits) for i in range(n_grp)])

    def blk_swap(a, bits):
        return lax.ppermute(a, "blk", [(i, i ^ bits) for i in range(n_blk)])

    turned = a_tiles.reshape(slots_here, PB, BS, BS).swapaxes(2, 3).reshape(a_tiles.shape)

    coded = jnp.stack([tile_codes >> 4, tile_codes & 15]).astype(jnp.bfloat16)
    coded = jnp.pad(coded, ((0, 14), (0, wide - slots_here)))
    small = jnp.concatenate([green_virt, green_occ, coded], axis=0)
    small = lax.all_gather(small, "grp", axis=1, tiled=True)
    turned, small = lax.optimization_barrier((turned, small))
    virt_all, occ_rows = small[:basis], small[basis : basis + lam]
    part = small[basis + lam : basis + lam + 2].reshape(-1, lam)
    code_rows = part.shape[0]
    part = jnp.pad(part, ((0, -code_rows % 16), (0, 0)))
    received = []
    for mask in range(n_blk):
        mine = lax.dynamic_slice_in_dim(occ_rows, (group ^ mask) * lam, lam, 1)
        packet = jnp.concatenate([mine, part], axis=0)
        received.append(blk_swap(packet, mask) if mask else packet)
    received = jnp.stack(received)
    occ = jnp.take(received[:, :lam], jnp.arange(n_blk, dtype=jnp.int32) ^ group, axis=0)
    occ = occ.reshape(basis, lam)
    part = received[:, lam : lam + code_rows].reshape(n_blk, 2, basis).astype(jnp.int32)
    codes = (part[:, 0] * 16 + part[:, 1]).reshape(-1)

    mask = lax.dynamic_slice_in_dim(occ_mask, group * KB, KB, 1)
    mask = jnp.repeat(jnp.repeat(mask, BS, axis=0), BS, axis=1).astype(jnp.bfloat16)
    occ = occ * mask
    occ = jnp.concatenate([occ[-(BAND - 1) * BS :], occ], axis=0)
    virt = jnp.concatenate([virt_all, virt_all[:, : (BAND - 1) * BS]], axis=1)
    virt = lax.dynamic_slice_in_dim(virt, group * lam, lam + (BAND - 1) * BS, 1)
    virt = jnp.stack([virt[:, l * BS : (l + BAND) * BS] for l in range(KB)])

    b = b3c.reshape(lam, BAND * BS, q)
    cols = min(2 * LANES, q)
    hops = []
    for d in range(1, spread):
        with jax.named_scope(f"hop{d}"):
            hops.append(grp_swap(turned, 2 * d))
    paired = [transform(b, virt, occ, cols, 0)]
    hops, paired = lax.optimization_barrier((hops, paired))
    near = {0: jnp.concatenate([turned] + hops)}
    bits = [1 << i for i in range((n_blk - 1).bit_length())]
    for to in bits:
        near[to] = blk_swap(near[0], to)
    far = {0: grp_swap(near[0], 1)}
    paired += [transform(b, virt, occ, cols, h) for h in range(1, q // cols)]
    chi = contract([near[0]], [far[0]], paired, codes, wide, slots_here, aux, (0,))
    arriving, chi = lax.optimization_barrier(([[near[to]] for to in bits], chi))
    sums = [chi]
    levels = [[m for m in range(n_blk) if m.bit_count() == n] for n in range(1, len(bits) + 1)]
    half = near[0].shape[0] // 2
    for masks, after in zip(levels, levels[1:] + [[]]):
        for to, pieces in zip(masks, arriving):
            near[to] = pieces[0] if len(pieces) == 1 else jnp.concatenate(pieces)
        arriving = []
        for to in after:
            low, high = to & -to, 1 << (to.bit_length() - 1)
            arriving.append(
                [blk_swap(near[to ^ low][:half], low), blk_swap(near[to ^ high][half:], high)]
            )
        for to in masks:
            far[to] = grp_swap(near[to], 1)
        chi = contract(
            [near[m] for m in masks],
            [far[m] for m in masks],
            paired,
            codes,
            wide,
            slots_here,
            aux,
            masks,
        )
        arriving, chi = lax.optimization_barrier((arriving, chi))
        sums.append(chi)

    def piece(d):
        rows = [lax.dynamic_slice_in_dim(chi, (group ^ d) * PBD, PBD, 0) for chi in sums]
        return sum(rows).reshape(PBD * PB, q)

    total = piece(0)
    for d in range(1, n_blk):
        total = total + blk_swap(piece(d).astype(jnp.bfloat16), d).astype(jnp.float32)
    return total


def solution(mesh):
    in_specs = (
        P("blk", None, None, "grp"),
        P("blk", "grp"),
        P(None, "grp"),
        P(),
        P(("blk", "grp"), None, None),
        P(("blk", "grp")),
    )
    out_specs = P("blk", "grp")
    return jax.shard_map(local, mesh=mesh, in_specs=in_specs, out_specs=out_specs, check_vma=False)
```

```python
import functools

import jax
import jax.numpy as jnp
from jax import lax
from jax.experimental import pallas as pl
from jax.experimental.pallas import tpu as pltpu
from jax.sharding import PartitionSpec as P


BS = 32
PB = 32
KB = 3
BAND = 3
PBD = 4
LANES = 128
NU_PART = 6
SUB = 2


def transform_kernel(pitch, begin, gv_ref, go_ref, b_ref, *refs):
    part, at_sub = pl.program_id(0) + begin, pl.program_id(1)
    halves = b_ref.shape[2] // LANES
    out_ref, scratch = refs[-1 - halves], refs[-halves:]
    rows = gv_ref.shape[1]
    lam = b_ref.shape[0]

    @pl.when(at_sub == 0)
    def _():
        for at in range(lam):
            r = jnp.dot(gv_ref[at // BS], b_ref[at], preferred_element_type=jnp.float32)
            for c, s in enumerate(scratch):
                s[pl.ds(at, rows, stride=pitch), :] = r[:, c * LANES : (c + 1) * LANES]

    for nb in range(SUB):
        here = at_sub * SUB + nb
        start = pl.multiple_of((part * (rows // BS) + here) * BS, BS)
        occ = go_ref[pl.ds(start, BAND * BS), :]
        zero = jnp.zeros_like(occ)
        occ = jnp.concatenate(
            [jnp.concatenate([occ, zero], axis=1), jnp.concatenate([zero, occ], axis=1)], axis=0
        )
        for i in range(BS // 2):
            at = (here * BS + 2 * i) * pitch
            w = jnp.concatenate(
                [
                    jnp.concatenate([s[pl.ds(at, lam), :], s[pl.ds(at + pitch, lam), :]], axis=0)
                    for s in scratch
                ],
                axis=1,
            )
            r = jnp.dot(occ, w.astype(jnp.bfloat16), preferred_element_type=jnp.float32)
            r = r.astype(jnp.bfloat16)
            for h in range(2):
                for j in range(BAND):
                    row = (h * BAND + j) * BS
                    to = (2 * i + h) * BS
                    out_ref[nb, BAND - 1 - j, to : to + BS, :] = r[row : row + BS]


def transform(b, gv, go, cols, which, begin, end, into=None):
    lam, band, _ = b.shape
    nb_total = gv.shape[1] // BS
    rows = NU_PART * BS
    pitch = lam + 2
    subs = NU_PART // SUB
    held = [] if into is None else [into]
    return pl.pallas_call(
        functools.partial(transform_kernel, pitch, begin),
        grid=(end - begin, subs),
        in_specs=[
            pl.BlockSpec((lam // BS, rows, band), lambda j, i: (0, j + begin, 0)),
            pl.BlockSpec(go.shape, lambda j, i: (0, 0)),
            pl.BlockSpec((lam, band, cols), lambda j, i: (0, 0, which)),
        ]
        + [pl.BlockSpec(memory_space=pl.ANY)] * len(held),
        out_specs=pl.BlockSpec(
            (SUB, BAND, BS * BS, cols), lambda j, i: ((j + begin) * subs + i, 0, 0, 0)
        ),
        out_shape=jax.ShapeDtypeStruct((nb_total, BAND, BS * BS, cols), jnp.bfloat16),
        scratch_shapes=[pltpu.VMEM((rows * pitch, LANES), jnp.float32)] * (cols // LANES),
        input_output_aliases={3: 0} if held else {},
        compiler_params=pltpu.CompilerParams(vmem_limit_bytes=62 * 2**20),
        cost_estimate=pl.CostEstimate(
            flops=75 * 10**8 * (end - begin), bytes_accessed=12 * 2**20, transcendentals=0
        ),
        name="transform",
    )(gv, go, b, *held)


def tiles_kernel(masks, halves, code_ref, *refs):
    groups, pairs = len(masks), KB * BAND
    sources, paired = refs[: 2 * groups], refs[2 * groups : 2 * groups + halves]
    out_ref, tiles, rhs, table, count, jobs, tile_sem, pair_sem = refs[-8:]
    aux = out_ref.shape[0] - 1
    slots = tiles.shape[2]
    cols = rhs.shape[3]
    group = lax.axis_index("blk")
    blocks = paired[0].shape[0]

    def tile_copy(g, side):
        return pltpu.make_async_copy(sources[2 * g + side], tiles.at[g, side], tile_sem.at[g, side])

    def pair_copy(mask, at, p, h):
        nu = lax.rem((group ^ mask) * KB + p // BAND + p % BAND, blocks)
        return pltpu.make_async_copy(
            paired[h].at[nu, p % BAND], rhs.at[at, h], pair_sem.at[at, h]
        )

    for g, mask in enumerate(masks):
        for side in range(2):
            tile_copy(g, side).start()
        for p in range(pairs):
            for h in range(halves):
                pair_copy(mask, g * pairs + p, p, h).start()
    out_ref[...] = jnp.zeros_like(out_ref)
    for at in range(groups * pairs * 2):
        count[at] = 0
    jobs[0] = 0
    for g, mask in enumerate(masks):
        for side in range(2):

            def put(s, carry):
                code = code_ref[(mask * 2 + side) * slots + s]

                @pl.when(code >= 0)
                def _():
                    at = (g * pairs + lax.rem(code, pairs)) * 2 + side
                    n = count[at]
                    table[at * slots + n] = lax.div(code, pairs) * 256 + s
                    count[at] = n + 1

                    @pl.when((n > 1) & (n % 2 == 0) & ((side == 0) | (count[at - side] <= n)))
                    def _():
                        jobs[0] = jobs[0] + 1
                        jobs[jobs[0]] = at // 2 * 256 + n // 2

                return carry

            lax.fori_loop(0, slots, put, 0)

    def item(g, pair, i):
        rows, lhs = [], []
        for side in range(2):
            for n in (2 * i, 2 * i + 1):
                at = pair * 2 + side
                entry = jnp.where(n < count[at], table[at * slots + n], aux * 256)
                rows.append(entry >> 8)
                lhs.append(tiles[g, side, entry & 255])
        lhs = jnp.concatenate(lhs, axis=0)
        for h in range(halves):
            r = jnp.dot(lhs, rhs[pair, h], preferred_element_type=jnp.float32)
            for t in range(4):
                out_ref[rows[t], :, h * cols : (h + 1) * cols] += r[t * PB : (t + 1) * PB]

    for g, mask in enumerate(masks):
        for side in range(2):
            tile_copy(g, side).wait()
        for p in range(pairs):
            for h in range(halves):
                pair_copy(mask, g * pairs + p, p, h).wait()
        for p in range(pairs):
            item(g, g * pairs + p, 0)

    def again(job, carry):
        pair = jobs[job] >> 8
        item(lax.div(pair, pairs), pair, jobs[job] & 255)
        return carry

    lax.fori_loop(1, jobs[0] + 1, again, 0)


def contract(near, far, paired, codes, aux, masks):
    halves = len(paired)
    cols = paired[0].shape[3]
    q = halves * cols
    groups, pairs = len(masks), KB * BAND
    slots = near[0].shape[0]
    acc = pl.BlockSpec((aux + 1, PB, q), lambda i, *_: (0, 0, 0))
    far_memory = pl.BlockSpec(memory_space=pltpu.HBM)
    return pl.pallas_call(
        functools.partial(tiles_kernel, masks, halves),
        grid_spec=pltpu.PrefetchScalarGridSpec(
            num_scalar_prefetch=1,
            grid=(1,),
            in_specs=[far_memory] * (2 * groups + halves),
            out_specs=acc,
            scratch_shapes=[
                pltpu.VMEM((groups, 2) + near[0].shape, jnp.bfloat16),
                pltpu.VMEM((groups * pairs, halves, BS * BS, cols), jnp.bfloat16),
                pltpu.SMEM((groups * pairs * 2 * slots,), jnp.int32),
                pltpu.SMEM((groups * pairs * 2,), jnp.int32),
                pltpu.SMEM((groups * slots + 1,), jnp.int32),
                pltpu.SemaphoreType.DMA((groups, 2)),
                pltpu.SemaphoreType.DMA((groups * pairs, halves)),
            ],
        ),
        out_shape=jax.ShapeDtypeStruct((aux + 1, PB, q), jnp.float32),
        compiler_params=pltpu.CompilerParams(vmem_limit_bytes=62 * 2**20),
        cost_estimate=pl.CostEstimate(
            flops=40 * 10**8 * groups, bytes_accessed=12 * 2**20 * groups, transcendentals=0
        ),
        name="contract",
    )(
        codes,
        *[side for pair in zip(near, far) for side in pair],
        *paired,
    )


def local(b3c, green_occ, green_virt, occ_mask, a_tiles, tile_codes):
    n_blk, n_grp = lax.axis_size("blk"), lax.axis_size("grp")
    group, member = lax.axis_index("blk"), lax.axis_index("grp")
    lam, _, _, q = b3c.shape
    basis, wide = green_virt.shape
    blocks = basis // BS
    aux = n_blk * PBD
    slots_here = a_tiles.shape[0]
    spread = n_grp // 2

    def grp_swap(a, bits):
        return lax.ppermute(a, "grp", [(i, i ^ bits) for i in range(n_grp)])

    def blk_swap(a, bits):
        return lax.ppermute(a, "blk", [(i, i ^ bits) for i in range(n_blk)])

    turned = a_tiles.reshape(slots_here, PB, BS, BS).swapaxes(2, 3).reshape(a_tiles.shape)

    coded = jnp.stack([tile_codes >> 4, tile_codes & 15]).astype(jnp.bfloat16)
    coded = jnp.pad(coded, ((0, 14), (0, wide - slots_here)))
    small = jnp.concatenate([green_virt, green_occ, coded], axis=0)[None]
    bit = 2
    while bit < n_grp:
        moved = grp_swap(small, bit)
        small = jnp.concatenate([small, moved], axis=0)
        bit *= 2
    small = jnp.concatenate([small, grp_swap(small, 1)], axis=0)
    relative = jnp.arange(n_grp, dtype=jnp.int32) ^ member
    order = relative % 2 * spread + relative // 2
    ordered = jnp.take(small[:, : basis + lam], order, axis=0)
    virt_all = ordered[:, :basis].swapaxes(0, 1).reshape(basis, basis)
    occ_rows = ordered[:, basis:].swapaxes(0, 1).reshape(lam, basis)
    code_rows = -(-2 * n_grp * slots_here // (16 * lam)) * 16
    part = small[:, basis + lam : basis + lam + 2, :slots_here].swapaxes(0, 1).reshape(2, -1)
    part = jnp.pad(part, ((0, 0), (0, code_rows // 2 * lam - part.shape[1])))
    part = part.reshape(code_rows, lam)
    received = []
    for mask in range(n_blk):
        mine = lax.dynamic_slice_in_dim(occ_rows, (group ^ mask) * lam, lam, 1)
        packet = jnp.concatenate([mine, part], axis=0)
        received.append(blk_swap(packet, mask) if mask else packet)
    received = jnp.stack(received)
    occ = jnp.take(received[:, :lam], jnp.arange(n_blk, dtype=jnp.int32) ^ group, axis=0)
    occ = occ.reshape(basis, lam)
    part = received[:, lam:].reshape(n_blk, 2, -1)[:, :, : n_grp * slots_here].astype(jnp.int32)
    codes = (part[:, 0] * 16 + part[:, 1]).reshape(-1)

    mask = lax.dynamic_slice_in_dim(occ_mask, group * KB, KB, 1)
    mask = jnp.repeat(jnp.repeat(mask, BS, axis=0), BS, axis=1).astype(jnp.bfloat16)
    occ = occ * mask
    occ = jnp.concatenate([occ[-(BAND - 1) * BS :], occ], axis=0)
    virt = jnp.concatenate([virt_all, virt_all[:, : (BAND - 1) * BS]], axis=1)
    virt = lax.dynamic_slice_in_dim(virt, group * lam, lam + (BAND - 1) * BS, 1)
    virt = jnp.stack([virt[:, l * BS : (l + BAND) * BS] for l in range(KB)])

    b = b3c.reshape(lam, BAND * BS, q)
    cols = min(2 * LANES, q)
    hops = []
    for d in range(1, spread):
        hops.append(grp_swap(turned, 2 * d))
    paired = transform(b, virt, occ, cols, 0, 0, 1)
    hops, paired = lax.optimization_barrier((hops, paired))
    near = {0: jnp.concatenate([turned] + hops)}
    for to in range(1, n_blk):
        near[to] = blk_swap(near[0], to)
    paired = [transform(b, virt, occ, cols, 0, 1, blocks // NU_PART, paired)]
    for h in range(1, q // cols):
        paired.append(transform(b, virt, occ, cols, h, 0, blocks // NU_PART))
    sums = []
    for at in range(0, n_blk, 3):
        masks = range(at, min(at + 3, n_blk))
        mine = [near[m] for m in masks]
        if sums:
            mine, sums[-1] = lax.optimization_barrier((mine, sums[-1]))
            far = []
        else:
            far = [grp_swap(mine[0], 1)]
            mine[1:], paired = lax.optimization_barrier((mine[1:], paired))
        far += [grp_swap(tiles, 1) for tiles in mine[len(far) :]]
        sums.append(contract(mine, far, paired, codes, aux, masks))

    def piece(d):
        rows = [lax.dynamic_slice_in_dim(chi, (group ^ d) * PBD, PBD, 0) for chi in sums]
        return sum(rows).reshape(PBD * PB, q)

    total = piece(0)
    for d in range(1, n_blk):
        total = total + blk_swap(piece(d).astype(jnp.bfloat16), d).astype(jnp.float32)
    return total


def solution(mesh):
    in_specs = (
        P("blk", None, None, "grp"),
        P("blk", "grp"),
        P(None, "grp"),
        P(),
        P(("blk", "grp"), None, None),
        P(("blk", "grp")),
    )
    out_specs = P("blk", "grp")
    return jax.shard_map(local, mesh=mesh, in_specs=in_specs, out_specs=out_specs, check_vma=False)
```

```python
import functools

import jax
import jax.numpy as jnp
from jax import lax
from jax.experimental import pallas as pl
from jax.experimental.pallas import tpu as pltpu
from jax.sharding import PartitionSpec as P


BS = 32
PB = 32
KB = 3
BAND = 3
PBD = 4
LANES = 128
NU_PART = 6
SUB = 2


def transform_kernel(pitch, begin, gv_ref, go_ref, b_ref, *refs):
    part, at_sub = pl.program_id(0) + begin, pl.program_id(1)
    halves = b_ref.shape[2] // LANES
    out_ref, scratch = refs[-1 - halves], refs[-halves:]
    rows = gv_ref.shape[1]
    lam = b_ref.shape[0]

    @pl.when(at_sub == 0)
    def _():
        for at in range(lam):
            r = jnp.dot(gv_ref[at // BS], b_ref[at], preferred_element_type=jnp.float32)
            for c, s in enumerate(scratch):
                s[pl.ds(at, rows, stride=pitch), :] = r[:, c * LANES : (c + 1) * LANES]

    for nb in range(SUB):
        here = at_sub * SUB + nb
        start = pl.multiple_of((part * (rows // BS) + here) * BS, BS)
        occ = go_ref[pl.ds(start, BAND * BS), :]
        zero = jnp.zeros_like(occ)
        occ = jnp.concatenate(
            [jnp.concatenate([occ, zero], axis=1), jnp.concatenate([zero, occ], axis=1)], axis=0
        )
        for i in range(BS // 2):
            at = (here * BS + 2 * i) * pitch
            w = jnp.concatenate(
                [
                    jnp.concatenate([s[pl.ds(at, lam), :], s[pl.ds(at + pitch, lam), :]], axis=0)
                    for s in scratch
                ],
                axis=1,
            )
            r = jnp.dot(occ, w.astype(jnp.bfloat16), preferred_element_type=jnp.float32)
            r = r.astype(jnp.bfloat16)
            for h in range(2):
                for j in range(BAND):
                    row = (h * BAND + j) * BS
                    to = (2 * i + h) * BS
                    out_ref[nb, BAND - 1 - j, to : to + BS, :] = r[row : row + BS]


def transform(b, gv, go, cols, which, begin, end, into=None):
    lam, band, _ = b.shape
    nb_total = gv.shape[1] // BS
    rows = NU_PART * BS
    pitch = lam + 2
    subs = NU_PART // SUB
    held = [] if into is None else [into]
    return pl.pallas_call(
        functools.partial(transform_kernel, pitch, begin),
        grid=(end - begin, subs),
        in_specs=[
            pl.BlockSpec((lam // BS, rows, band), lambda j, i: (0, j + begin, 0)),
            pl.BlockSpec(go.shape, lambda j, i: (0, 0)),
            pl.BlockSpec((lam, band, cols), lambda j, i: (0, 0, which)),
        ]
        + [pl.BlockSpec(memory_space=pl.ANY)] * len(held),
        out_specs=pl.BlockSpec(
            (SUB, BAND, BS * BS, cols), lambda j, i: ((j + begin) * subs + i, 0, 0, 0)
        ),
        out_shape=jax.ShapeDtypeStruct((nb_total, BAND, BS * BS, cols), jnp.bfloat16),
        scratch_shapes=[pltpu.VMEM((rows * pitch, LANES), jnp.float32)] * (cols // LANES),
        input_output_aliases={3: 0} if held else {},
        compiler_params=pltpu.CompilerParams(vmem_limit_bytes=62 * 2**20),
        cost_estimate=pl.CostEstimate(
            flops=75 * 10**8 * (end - begin), bytes_accessed=12 * 2**20, transcendentals=0
        ),
        name="transform",
    )(gv, go, b, *held)


def tiles_kernel(masks, halves, code_ref, *refs):
    groups, pairs = len(masks), KB * BAND
    sources, paired = refs[: 2 * groups], refs[2 * groups : 2 * groups + halves]
    out_ref, tiles, rhs, table, count, jobs, tile_sem, pair_sem = refs[-8:]
    aux = out_ref.shape[0] - 1
    slots = tiles.shape[2]
    cols = rhs.shape[3]
    group = lax.axis_index("blk")
    blocks = paired[0].shape[0]

    def tile_copy(g, side):
        return pltpu.make_async_copy(sources[2 * g + side], tiles.at[g, side], tile_sem.at[g, side])

    def pair_copy(mask, at, p, h):
        nu = lax.rem((group ^ mask) * KB + p // BAND + p % BAND, blocks)
        return pltpu.make_async_copy(
            paired[h].at[nu, p % BAND], rhs.at[at, h], pair_sem.at[at, h]
        )

    for g, mask in enumerate(masks):
        for side in range(2):
            tile_copy(g, side).start()
        for p in range(pairs):
            for h in range(halves):
                pair_copy(mask, g * pairs + p, p, h).start()
    out_ref[...] = jnp.zeros_like(out_ref)
    for at in range(groups * pairs * 2):
        count[at] = 0
    jobs[0] = 0
    for g, mask in enumerate(masks):
        for side in range(2):

            def put(s, carry):
                code = code_ref[(mask * 2 + side) * slots + s]

                @pl.when(code >= 0)
                def _():
                    at = (g * pairs + lax.rem(code, pairs)) * 2 + side
                    n = count[at]
                    table[at * slots + n] = lax.div(code, pairs) * 256 + s
                    count[at] = n + 1

                    @pl.when((n > 1) & (n % 2 == 0) & ((side == 0) | (count[at - side] <= n)))
                    def _():
                        jobs[0] = jobs[0] + 1
                        jobs[jobs[0]] = at // 2 * 256 + n // 2

                return carry

            lax.fori_loop(0, slots, put, 0)

    def item(g, pair, i):
        rows, lhs = [], []
        for side in range(2):
            for n in (2 * i, 2 * i + 1):
                at = pair * 2 + side
                entry = jnp.where(n < count[at], table[at * slots + n], aux * 256)
                rows.append(entry >> 8)
                lhs.append(tiles[g, side, entry & 255])
        lhs = jnp.concatenate(lhs, axis=0)
        for h in range(halves):
            r = jnp.dot(lhs, rhs[pair, h], preferred_element_type=jnp.float32)
            for t in range(4):
                out_ref[rows[t], :, h * cols : (h + 1) * cols] += r[t * PB : (t + 1) * PB]

    for g, mask in enumerate(masks):
        for side in range(2):
            tile_copy(g, side).wait()
        for p in range(pairs):
            for h in range(halves):
                pair_copy(mask, g * pairs + p, p, h).wait()
        for p in range(pairs):
            item(g, g * pairs + p, 0)

    def again(job, carry):
        pair = jobs[job] >> 8
        item(lax.div(pair, pairs), pair, jobs[job] & 255)
        return carry

    lax.fori_loop(1, jobs[0] + 1, again, 0)


def contract(near, far, paired, codes, aux, masks):
    halves = len(paired)
    cols = paired[0].shape[3]
    q = halves * cols
    groups, pairs = len(masks), KB * BAND
    slots = near[0].shape[0]
    acc = pl.BlockSpec((aux + 1, PB, q), lambda i, *_: (0, 0, 0))
    far_memory = pl.BlockSpec(memory_space=pltpu.HBM)
    return pl.pallas_call(
        functools.partial(tiles_kernel, masks, halves),
        grid_spec=pltpu.PrefetchScalarGridSpec(
            num_scalar_prefetch=1,
            grid=(1,),
            in_specs=[far_memory] * (2 * groups + halves),
            out_specs=acc,
            scratch_shapes=[
                pltpu.VMEM((groups, 2) + near[0].shape, jnp.bfloat16),
                pltpu.VMEM((groups * pairs, halves, BS * BS, cols), jnp.bfloat16),
                pltpu.SMEM((groups * pairs * 2 * slots,), jnp.int32),
                pltpu.SMEM((groups * pairs * 2,), jnp.int32),
                pltpu.SMEM((groups * slots + 1,), jnp.int32),
                pltpu.SemaphoreType.DMA((groups, 2)),
                pltpu.SemaphoreType.DMA((groups * pairs, halves)),
            ],
        ),
        out_shape=jax.ShapeDtypeStruct((aux + 1, PB, q), jnp.float32),
        compiler_params=pltpu.CompilerParams(vmem_limit_bytes=62 * 2**20),
        cost_estimate=pl.CostEstimate(
            flops=40 * 10**8 * groups, bytes_accessed=12 * 2**20 * groups, transcendentals=0
        ),
        name="contract",
    )(
        codes,
        *[side for pair in zip(near, far) for side in pair],
        *paired,
    )


def local(b3c, green_occ, green_virt, occ_mask, a_tiles, tile_codes):
    n_blk, n_grp = lax.axis_size("blk"), lax.axis_size("grp")
    group, member = lax.axis_index("blk"), lax.axis_index("grp")
    lam, _, _, q = b3c.shape
    basis, wide = green_virt.shape
    blocks = basis // BS
    aux = n_blk * PBD
    slots_here = a_tiles.shape[0]
    spread = n_grp // 2

    def grp_swap(a, bits):
        return lax.ppermute(a, "grp", [(i, i ^ bits) for i in range(n_grp)])

    def blk_swap(a, bits):
        return lax.ppermute(a, "blk", [(i, i ^ bits) for i in range(n_blk)])

    turned = a_tiles.reshape(slots_here, PB, BS, BS).swapaxes(2, 3).reshape(a_tiles.shape)

    coded = jnp.stack([tile_codes >> 4, tile_codes & 15]).astype(jnp.bfloat16)
    coded = jnp.pad(coded, ((0, 14), (0, wide - slots_here)))
    small = jnp.concatenate([green_virt, green_occ, coded], axis=0)[None]
    bit = 2
    while bit < n_grp:
        moved = grp_swap(small, bit)
        small = jnp.concatenate([small, moved], axis=0)
        bit *= 2
    small = jnp.concatenate([small, grp_swap(small, 1)], axis=0)
    relative = jnp.arange(n_grp, dtype=jnp.int32) ^ member
    order = relative % 2 * spread + relative // 2
    ordered = jnp.take(small[:, : basis + lam], order, axis=0)
    virt_all = ordered[:, :basis].swapaxes(0, 1).reshape(basis, basis)
    occ_rows = ordered[:, basis:].swapaxes(0, 1).reshape(lam, basis)
    code_rows = -(-2 * n_grp * slots_here // (16 * lam)) * 16
    part = small[:, basis + lam : basis + lam + 2, :slots_here].swapaxes(0, 1).reshape(2, -1)
    part = jnp.pad(part, ((0, 0), (0, code_rows // 2 * lam - part.shape[1])))
    part = part.reshape(code_rows, lam)
    received = []
    for mask in range(n_blk):
        mine = lax.dynamic_slice_in_dim(occ_rows, (group ^ mask) * lam, lam, 1)
        packet = jnp.concatenate([mine, part], axis=0)
        received.append(blk_swap(packet, mask) if mask else packet)
    received = jnp.stack(received)
    occ = jnp.take(received[:, :lam], jnp.arange(n_blk, dtype=jnp.int32) ^ group, axis=0)
    occ = occ.reshape(basis, lam)
    part = received[:, lam:].reshape(n_blk, 2, -1)[:, :, : n_grp * slots_here].astype(jnp.int32)
    codes = (part[:, 0] * 16 + part[:, 1]).reshape(-1)

    mask = lax.dynamic_slice_in_dim(occ_mask, group * KB, KB, 1)
    mask = jnp.repeat(jnp.repeat(mask, BS, axis=0), BS, axis=1).astype(jnp.bfloat16)
    occ = occ * mask
    occ = jnp.concatenate([occ[-(BAND - 1) * BS :], occ], axis=0)
    virt = jnp.concatenate([virt_all, virt_all[:, : (BAND - 1) * BS]], axis=1)
    virt = lax.dynamic_slice_in_dim(virt, group * lam, lam + (BAND - 1) * BS, 1)
    virt = jnp.stack([virt[:, l * BS : (l + BAND) * BS] for l in range(KB)])

    b = b3c.reshape(lam, BAND * BS, q)
    cols = min(2 * LANES, q)
    hops = []
    for d in range(1, spread):
        hops.append(grp_swap(turned, 2 * d))
    paired = transform(b, virt, occ, cols, 0, 0, 1)
    hops, paired = lax.optimization_barrier((hops, paired))
    near = {0: jnp.concatenate([turned] + hops)}
    for to in range(1, n_blk):
        near[to] = blk_swap(near[0], to)
    paired = [transform(b, virt, occ, cols, 0, 1, blocks // NU_PART, paired)]
    for h in range(1, q // cols):
        paired.append(transform(b, virt, occ, cols, h, 0, blocks // NU_PART))
    sums = []
    for at in range(0, n_blk, 2):
        masks = range(at, at + 2)
        mine = [near[m] for m in masks]
        if sums:
            far = []
            for i, tiles in enumerate(mine):
                mine[i], sums[-1], far = lax.optimization_barrier((tiles, sums[-1], far))
                far.append(grp_swap(mine[i], 1))
        else:
            far = [grp_swap(mine[0], 1)]
            mine[1:], paired = lax.optimization_barrier((mine[1:], paired))
        far += [grp_swap(tiles, 1) for tiles in mine[len(far) :]]
        sums.append(contract(mine, far, paired, codes, aux, masks))

    def piece(d):
        rows = [lax.dynamic_slice_in_dim(chi, (group ^ d) * PBD, PBD, 0) for chi in sums]
        return sum(rows).reshape(PBD * PB, q)

    total = piece(0)
    for d in range(1, n_blk):
        total = total + blk_swap(piece(d).astype(jnp.bfloat16), d).astype(jnp.float32)
    return total


def solution(mesh):
    in_specs = (
        P("blk", None, None, "grp"),
        P("blk", "grp"),
        P(None, "grp"),
        P(),
        P(("blk", "grp"), None, None),
        P(("blk", "grp")),
    )
    out_specs = P("blk", "grp")
    return jax.shard_map(local, mesh=mesh, in_specs=in_specs, out_specs=out_specs, check_vma=False)
```
